128 devices in a mesh: row: 8 (over z, core), col: 16 (over x, y).
Axes of the slice: x: 4, y: 4, z: 4, core: 2. Of those that a mesh axis runs over, the one named last changes fastest.
Arguments:
- activations: bfloat16 [8192, 8192], P('row', 'col'), may hold values from -6 to 6
- errors: bfloat16 [8192, 8192], P('row', 'col'), may hold values from -6 to 6
- act_proj: bfloat16 [8192, 128], P('col'), may hold values from -0.0625 to 0.0625
- err_proj: bfloat16 [8192, 128], P('col'), may hold values from -0.0625 to 0.0625
- lengths: int32 [8, 64], P('row'), may hold values from 1 to 256, 1024 in all within a row
- ridge: float32 [16384, 16384], P('row', 'col'), may hold values from -4 to 36, as said below
- pivot_inverse: float32 [2, 512, 512], replicated, may hold values from -1 to 1
Outputs:
- eliminated: float32 [16384, 16384], P('row', 'col')
The draws below stay inside these ranges and needn't reach their ends.
Inputs may be any that keep to these rules, and one draw needn't show every extreme that they name: The lengths of one row group sum to 1024. `ridge`: Symmetric.
All inputs are finite; a program needn't handle non-finite values.
Results may differ from the reference program's by a relative error of at most 0.0074.
Values may be sent and summed in bfloat16 or wider, within the bound.
A program may use at most 128 MiB of HBM per device.

```python
import math
import jax
import jax.numpy as jnp
import numpy as np
from jax import lax

D = 8192
PROJ = 128
PANEL = 512
CAP_DEV = 64
TOK_DEV = 1024
CAPTIONS = 512
TOKENS = 8192
ORDER = 16384
N_ROW = 8


def draw_ridge(key, part):
    order = PROJ * PROJ
    key_diag, key_off = jax.random.split(jax.random.fold_in(key, 11))
    diagonal = jnp.exp(jax.random.uniform(key_diag, (order,), jnp.float32, math.log(8.0), math.log(32.0)))
    uniform_part = jax.random.uniform(key_off, (order, order), jnp.float32, -1.0, 1.0)
    symmetric = 2.0 * (uniform_part + uniform_part.T)
    return symmetric + jnp.diag(diagonal)


def draw_pivot_inverse(key, part):
    key_diag, key_off = jax.random.split(jax.random.fold_in(key, 23))
    diagonal = jnp.exp(jax.random.uniform(key_diag, (2, PANEL), jnp.float32, math.log(0.06), math.log(0.15)))
    strict_lower = jax.random.truncated_normal(key_off, -4.0, 4.0, (2, PANEL, PANEL), jnp.float32) * (0.03 / math.sqrt(PANEL))
    lower_mask = jnp.tril(jnp.ones((PANEL, PANEL), jnp.float32), -1)
    return strict_lower * lower_mask[None] + diagonal[:, :, None] * jnp.eye(PANEL, dtype=jnp.float32)[None]


def level_of(rng, dims, pieces, low, top_value):
    factor_of, own = 1.0, jax.random.fold_in(rng, 6)
    for dim, parts in pieces:
        draws = jnp.exp(jax.random.uniform(jax.random.fold_in(own, dim), (parts,), jnp.float32, low / len(pieces), top_value / len(pieces)))
        factor_of = factor_of * jnp.repeat(draws, dims[dim] // parts).reshape([-1 if axis == dim else 1 for axis in range(len(dims))])
    return factor_of


def profile(count, total, most, skew):
    loads = [(1 << 20) // math.isqrt(standing ** skew) + 1 for standing in range(2, count + 1)]
    spare, holding = total - most - (count - 1), [1] * (count - 1)
    while spare > 0:
        movable = [i for i in range(count - 1) if holding[i] < most]
        whole, remaining = sum([loads[i] for i in movable]), spare
        for i in movable:
            more = min(most - holding[i], max(1, remaining * loads[i] // whole), spare)
            holding[i] = holding[i] + more
            spare = spare - more
    return np.array([most] + holding)


def ragged_sizes(own_key, amount, total, reach, skew):
    if amount == 2:
        one = jax.random.randint(own_key, (), max(1, total - reach), min(reach, total - 1) + 1)
        return jnp.stack([one, total - one])
    sizes = jnp.asarray(profile(amount, total, reach, skew), jnp.int32)
    pairs = (amount - 1) // 2
    donor, taker = sizes[1:1 + 2 * pairs:2], sizes[2:2 + 2 * pairs:2]
    margin = jnp.minimum(donor - 1, reach - taker)
    moved = jax.random.randint(jax.random.fold_in(own_key, 1), (pairs,), 0, 1 << 20) % (margin + 1)
    sizes = sizes.at[1:1 + 2 * pairs:2].set(donor - moved).at[2:2 + 2 * pairs:2].set(taker + moved)
    return sizes[jax.random.permutation(jax.random.fold_in(own_key, 2), amount)]


def noise(key, shape, scale, reach, cuts=(), kind=jnp.bfloat16):
    result = scale * jax.random.normal(key, shape, jnp.float32)
    if cuts:
        result = result * level_of(key, shape, cuts, -0.22, 0.18)
    return jnp.clip(result, -reach, reach).astype(kind)


def setup_inputs(seed: int = 0) -> dict:
    seeds = jax.random.split(jax.random.key(seed), 8)
    return {
        "activations": noise(seeds[0], (TOKENS, D), 1.0, 6.0, ((0, 8), (1, 16))),
        "errors": noise(seeds[1], (TOKENS, D), 1.0, 6.0, ((0, 8), (1, 16))),
        "act_proj": noise(seeds[2], (D, PROJ), D ** -0.5, 0.0625, ((0, 16),)),
        "err_proj": noise(seeds[3], (D, PROJ), D ** -0.5, 0.0625, ((0, 16),)),
        "lengths": jax.vmap(lambda own: ragged_sizes(own, CAP_DEV, TOK_DEV, TOK_DEV // 4, 2))(jax.random.split(seeds[4], N_ROW)).reshape((N_ROW, CAP_DEV)).astype(jnp.int32),
        "ridge": draw_ridge(jax.random.fold_in(seeds[7], 71), 0),
        "pivot_inverse": draw_pivot_inverse(jax.random.fold_in(seeds[7], 71), 0),
    }


def group_grads(inputs):
    proj_err, proj_act, lengths_row = inputs
    caption_end = jnp.cumsum(lengths_row).astype(jnp.int32)
    caption_start = (caption_end - lengths_row).astype(jnp.int32)
    positions = jnp.arange(TOK_DEV, dtype=jnp.int32)[:, None]
    member = ((positions >= caption_start[None, :]) & (positions < caption_end[None, :])).astype(jnp.float32)
    weighted = (proj_err.astype(jnp.float32)[:, :, None] * member[:, None, :]).reshape(TOK_DEV, PROJ * CAP_DEV)
    summed = jnp.dot(weighted.T, proj_act.astype(jnp.float32), precision=lax.Precision.HIGHEST)
    summed = summed.reshape(PROJ, CAP_DEV, PROJ).transpose(1, 0, 2).reshape(CAP_DEV, PROJ * PROJ)
    return summed.astype(jnp.bfloat16)


def reference(activations, errors, act_proj, err_proj, lengths, ridge, pivot_inverse):
    proj_act = jnp.dot(activations, act_proj, preferred_element_type=jnp.float32).astype(jnp.bfloat16)
    proj_err = jnp.dot(errors, err_proj, preferred_element_type=jnp.float32).astype(jnp.bfloat16)
    grads = lax.map(group_grads, (proj_err.reshape(N_ROW, TOK_DEV, PROJ), proj_act.reshape(N_ROW, TOK_DEV, PROJ), lengths))
    grads = grads.reshape(CAPTIONS, ORDER).astype(jnp.float32)
    matrix = ridge + jnp.dot(grads.T, grads, precision=lax.Precision.HIGHEST) / CAPTIONS
    row_ids = jnp.arange(ORDER, dtype=jnp.int32)[:, None]
    for panel_index in range(2):
        start_col = panel_index * PANEL
        stop_col = start_col + PANEL
        panel = jnp.dot(matrix[:, start_col:stop_col], pivot_inverse[panel_index].T, precision=lax.Precision.HIGHEST)
        panel = jnp.where(row_ids >= start_col, panel, 0.0)
        tail_rows = panel[stop_col:]
        matrix = matrix.at[stop_col:, stop_col:].add(-jnp.dot(tail_rows, tail_rows.T, precision=lax.Precision.HIGHEST))
        matrix = matrix.at[:, start_col:stop_col].set(panel)
        matrix = matrix.at[start_col:stop_col, stop_col:].set(0.0)
    return matrix
```

```python
import jax
import jax.numpy as jnp
from jax import lax
from jax.experimental import pallas as pl
from jax.experimental.pallas import tpu as pltpu
from jax.sharding import PartitionSpec as P

MESH = pl.DeviceIdType.MESH
BF = jnp.bfloat16
F32 = jnp.float32
CH = 16
VMEM_LIMIT = 66000000


def dot(a, b):
    return jnp.dot(a, b, preferred_element_type=F32)


def rcopy(src, dst, ssem, rsem, r, c):
    return pltpu.make_async_remote_copy(
        src_ref=src, dst_ref=dst, send_sem=ssem, recv_sem=rsem, device_id=(r, c), device_id_type=MESH
    )


def flip(v, bit):
    return v + 1 - 2 * (v % 2) if bit == 0 else 3 - v


def exchange(
    pact, perr, cap, ridge,
    act_o, erow_o, ecol_o, epan_o, cap_o, rows_o, colp_o, r01_o,
    act, erow, ecol, epan, capall, rows, colp, r01, rs_act, rs_err, my_act, my_err, stage,
    rs_s, rs_r, sa_s, sa_r, se_s, se_r, cp_s, cp_r,
    cz_s, cz_r, cd_s, cd_r, b1_s, b1_r, b2_s, b2_r,
    e1_s, e1_r, e2_s, e2_r, p1_s, p1_r, p2_s, p2_r, d2_s, d2_r,
    ts, tr, ld, loc, outs,
):
    r = lax.axis_index("row")
    c = lax.axis_index("col")
    z, k = r // 2, r % 2
    x, y = c // 4, c % 4
    partner = 2 * z + 1 - k

    def row_of(dz, dk):
        return 2 * ((z + dz) % 4) + (k + dk) % 2

    def xcol(d):
        return 4 * ((x + d) % 4) + y

    def ycol(d):
        return 4 * x + (y + d) % 4

    column = [(dz, dk) for dz in range(4) for dk in range(2) if dz or dk]
    loads = [
        pltpu.make_async_copy(ridge.at[pl.ds(n * 256, 256)], stage.at[pl.ds(n * 256, 256)], ld.at[n])
        for n in range(8)
    ]

    @pl.when(jnp.logical_or(c == 0, r == 0))
    def _():
        for copy in loads:
            copy.start()

    barrier = pltpu.get_barrier_semaphore()
    for d in range(1, 16):
        pl.semaphore_signal(barrier, inc=1, device_id=(r, (c + d) % 16), device_id_type=MESH)
    for dz, dk in column:
        pl.semaphore_signal(barrier, inc=1, device_id=(row_of(dz, dk), c), device_id_type=MESH)
    pl.semaphore_wait(barrier, 22)

    sends = []

    def go(copy):
        copy.start()
        sends.append(copy)

    for d in range(1, 16):
        to = (c + d) % 16
        go(rcopy(pact.at[to], rs_act.at[d], rs_s.at[0, d], rs_r.at[0, d], r, to))
        go(rcopy(perr.at[to], rs_err.at[d], rs_s.at[1, d], rs_r.at[1, d], r, to))
    for dz, dk in column:
        n = 2 * dz + dk
        go(rcopy(cap.at[0], capall.at[r], cp_s.at[n], cp_r.at[n], row_of(dz, dk), c))
    own_cap = pltpu.make_async_copy(cap.at[0], capall.at[r], loc.at[0])
    own_cap.start()

    @pl.when(jnp.logical_or(c == 0, r == 0))
    def _():
        for copy in loads:
            copy.wait()

    @pl.when(c == 0)
    def _():
        @pl.loop(0, 32)
        def _(n):
            part = pl.ds(pl.multiple_of(n * 64, 64), 64)
            rows[part, :] = stage[part, :].astype(BF)

    @pl.when(r == 0)
    def _():
        @pl.loop(0, 16)
        def _(n):
            part = pl.ds(pl.multiple_of(n * 64, 64), 64)
            colp[part, :] = stage[part, :].astype(BF)

    sum_act = pact[c].astype(F32)
    sum_err = perr[c].astype(F32)
    for d in range(1, 16):
        rcopy(pact.at[c], rs_act.at[d], rs_s.at[0, d], rs_r.at[0, d], partner, c).wait_recv()
        rcopy(perr.at[c], rs_err.at[d], rs_s.at[1, d], rs_r.at[1, d], partner, c).wait_recv()
        sum_act += rs_act[d].astype(F32)
        sum_err += rs_err[d].astype(F32)
    my_act[...] = sum_act.astype(BF)
    my_err[...] = sum_err.astype(BF)

    h, half = z // 2, z % 2
    slot = jnp.where(half == 0, 4 * y + x, c)
    mine = act.at[h, half, slot, k]
    own_act = pltpu.make_async_copy(my_act, mine, loc.at[1])
    own_err = pltpu.make_async_copy(my_err, ecol.at[r], loc.at[2])
    own_err.start()

    @pl.when(h == k)
    def _():
        own_act.start()

    @pl.when(h != k)
    def _():
        rcopy(my_act, mine, sa_s.at[0], sa_r.at[half, k], partner, c).start()

    for dz in range(1, 4):
        go(rcopy(my_act, mine, sa_s.at[dz], sa_r.at[half, k], 2 * ((z + dz) % 4) + h, c))
    for dz, dk in column:
        n = 2 * dz + dk
        go(rcopy(my_err, ecol.at[r], se_s.at[n], se_r.at[n], row_of(dz, dk), c))

    def piece(chain, n):
        return colp.at[pl.ds(chain * 512 + n * 128, 128)]

    @pl.when(k == 0)
    def _():
        for n in range(4):
            for chain in range(2):
                place = z if chain == 0 else (4 - z) % 4
                follow = 2 * ((z + 1) % 4) if chain == 0 else 2 * ((z + 3) % 4)
                copy = rcopy(
                    piece(chain, n), piece(chain, n), cz_s.at[chain, n], cz_r.at[chain, n], follow, c
                )

                @pl.when(place > 0)
                def _():
                    copy.wait_recv()

                @pl.when(place < 3)
                def _():
                    copy.start()

                rcopy(
                    piece(chain, n), piece(chain, n), cd_s.at[chain, n], cd_r.at[chain, n], partner, c
                ).start()

    for i in range(2):
        for j in range(2):
            away = jnp.logical_or(z != 2 * k + i, k != j)
            into = act.at[k, i, jnp.where(jnp.int32(i) == 0, 4 * y + x, c), j]

            @pl.when(away)
            def _():
                rcopy(my_act, into, sa_s.at[0], sa_r.at[i, j], partner, c).wait_recv()

    @pl.when(h == k)
    def _():
        own_act.wait()

    slot0, slot1 = 4 * y + x, c
    for d in range(1, 4):
        go(rcopy(act.at[k, 0, slot0], act.at[k, 0, slot0], b1_s.at[0, d], b1_r.at[0, d], r, xcol(d)))
        go(rcopy(act.at[k, 1, slot1], act.at[k, 1, slot1], b1_s.at[1, d], b1_r.at[1, d], r, ycol(d)))

    own_err.wait()
    for dz, dk in column:
        n = 2 * dz + dk
        rcopy(my_err, ecol.at[row_of(4 - dz, 2 - dk)], se_s.at[n], se_r.at[n], partner, c).wait_recv()

    in_rows = y // 2 == k
    e = y % 2
    row_src = jnp.logical_and(in_rows, x == z)
    pan_src = c == 0

    @pl.when(row_src)
    def _():
        for d in range(1, 4):
            rcopy(ecol, erow.at[e], e1_s.at[d], e1_r.at[0], r, xcol(d)).start()
        copy = pltpu.make_async_copy(ecol, erow.at[e], loc.at[3])
        copy.start()
        copy.wait()

    @pl.when(pan_src)
    def _():
        for d in range(1, 4):
            rcopy(ecol, epan, p1_s.at[d], p1_r.at[0], r, xcol(d)).start()
        copy = pltpu.make_async_copy(ecol, epan, loc.at[4])
        copy.start()
        copy.wait()

    @pl.when(jnp.logical_and(in_rows, x != z))
    def _():
        rcopy(ecol, erow.at[e], e1_s.at[0], e1_r.at[0], r, xcol(1)).wait_recv()

    @pl.when(in_rows)
    def _():
        for d in range(1, 4):
            rcopy(erow.at[e], erow.at[e], e2_s.at[d], e2_r.at[e], r, ycol(d)).start()

    @pl.when(jnp.logical_and(y == 0, x != 0))
    def _():
        rcopy(ecol, epan, p1_s.at[0], p1_r.at[0], r, xcol(1)).wait_recv()

    @pl.when(y == 0)
    def _():
        for d in range(1, 4):
            rcopy(epan, epan, p2_s.at[d], p2_r.at[0], r, ycol(d)).start()

    for d in range(1, 4):
        from_x = 4 * y + (x + 4 - d) % 4
        from_y = 4 * x + (y + 4 - d) % 4
        rcopy(act.at[k, 0, slot0], act.at[k, 0, from_x], b1_s.at[0, d], b1_r.at[0, d], r, xcol(d)).wait_recv()
        rcopy(act.at[k, 1, slot1], act.at[k, 1, from_y], b1_s.at[1, d], b1_r.at[1, d], r, ycol(d)).wait_recv()
    g0, g1 = pl.ds(4 * y, 4), pl.ds(4 * x, 4)
    for d in range(1, 4):
        go(rcopy(act.at[k, 0, g0], act.at[k, 0, g0], b2_s.at[0, d], b2_r.at[0, d], r, ycol(d)))
        go(rcopy(act.at[k, 1, g1], act.at[k, 1, g1], b2_s.at[1, d], b2_r.at[1, d], r, xcol(d)))

    @pl.when(k == 1)
    def _():
        for n in range(4):
            for chain in range(2):
                rcopy(
                    piece(chain, n), piece(chain, n), cd_s.at[chain, n], cd_r.at[chain, n], partner, c
                ).wait_recv()

    @pl.when(c == 0)
    def _():
        copy = pltpu.make_async_copy(colp.at[pl.ds(0, 512), pl.ds(512, 512)], r01, loc.at[5])
        copy.start()
        copy.wait()

    bits = [((x + 1) // 2) % 2, ((y + 1) // 2) % 2, x // 2, y // 2]
    count = bits[0] + bits[1] + bits[2] + bits[3]
    nbr = [4 * flip(x, 0) + y, 4 * x + flip(y, 0), 4 * flip(x, 1) + y, 4 * x + flip(y, 1)]
    tree = []
    for d in range(4):
        d1, d2, d3 = (d + 1) % 4, (d + 2) % 4, (d + 3) % 4
        up = jnp.where(bits[d1] == 1, d1, jnp.where(bits[d2] == 1, d2, jnp.where(bits[d3] == 1, d3, d)))
        tree.append(jnp.where(bits[d] == 1, d, up))
    sends_on = [jnp.logical_or(bits[d] == 0, count > 1) for d in range(4)]
    ch = 512 // CH

    def chunk(t, q):
        return rows.at[pl.ds(pl.multiple_of(t * 512 + q * ch, ch), ch)]

    def quarter(t):
        return r01.at[pl.ds(pl.multiple_of(t * 128, 128), 128)]

    def part_of(t, q):
        return quarter(t) if isinstance(q, int) else chunk(t, q)

    def relay(q):
        for t in range(4):

            @pl.when(bits[t] == 1)
            def _():
                rcopy(part_of(t, q), part_of(t, q), ts.at[0, q], tr.at[t, q], r, nbr[0]).wait_recv()

        for d in range(4):

            @pl.when(sends_on[d])
            def _():
                t = tree[d]
                rcopy(part_of(t, q), part_of(t, q), ts.at[d, q], tr.at[t, q], r, nbr[d]).start()

    def leaves(q):
        for t in range(4):

            @pl.when(jnp.logical_and(bits[t] == 0, count > 0))
            def _():
                rcopy(part_of(t, q), part_of(t, q), ts.at[0, q], tr.at[t, q], r, nbr[0]).wait_recv()

        for d in range(4):

            @pl.when(sends_on[d])
            def _():
                t = tree[d]
                rcopy(part_of(t, q), part_of(t, q), ts.at[d, q], tr.at[t, q], r, nbr[d]).wait_send()

    relay(CH)

    @pl.loop(0, CH)
    def _(q):
        relay(q)

    for d in range(1, 4):
        far0 = pl.ds(4 * ((y + 4 - d) % 4), 4)
        far1 = pl.ds(4 * ((x + 4 - d) % 4), 4)
        rcopy(act.at[k, 0, g0], act.at[k, 0, far0], b2_s.at[0, d], b2_r.at[0, d], r, ycol(d)).wait_recv()
        rcopy(act.at[k, 1, g1], act.at[k, 1, far1], b2_s.at[1, d], b2_r.at[1, d], r, xcol(d)).wait_recv()
    go(rcopy(act.at[k], act.at[k], d2_s, d2_r, partner, c))
    rcopy(act.at[k], act.at[1 - k], d2_s, d2_r, partner, c).wait_recv()

    for i in range(2):

        @pl.when(y != 2 * k + i)
        def _():
            rcopy(erow.at[i], erow.at[i], e2_s.at[0], e2_r.at[i], r, ycol(1)).wait_recv()

    @pl.when(y != 0)
    def _():
        rcopy(epan, epan, p2_s.at[0], p2_r.at[0], r, ycol(1)).wait_recv()

    own_cap.wait()
    for dz, dk in column:
        n = 2 * dz + dk
        rcopy(cap.at[0], capall.at[row_of(4 - dz, 2 - dk)], cp_s.at[n], cp_r.at[n], partner, c).wait_recv()

    leaves(CH)

    @pl.loop(0, CH)
    def _(q):
        leaves(q)

    pairs = (
        (act, act_o), (erow, erow_o), (ecol, ecol_o), (epan, epan_o),
        (capall, cap_o), (rows, rows_o), (colp, colp_o), (r01, r01_o),
    )
    done = [pltpu.make_async_copy(a, b, outs.at[n]) for n, (a, b) in enumerate(pairs)]
    for copy in done:
        copy.start()

    for copy in sends:
        copy.wait_send()

    @pl.when(h != k)
    def _():
        rcopy(my_act, mine, sa_s.at[0], sa_r.at[half, k], partner, c).wait_send()

    @pl.when(k == 0)
    def _():
        for n in range(4):
            for chain in range(2):
                place = z if chain == 0 else (4 - z) % 4
                copy = rcopy(
                    piece(chain, n), piece(chain, n), cz_s.at[chain, n], cz_r.at[chain, n], partner, c
                )

                @pl.when(place < 3)
                def _():
                    copy.wait_send()

                rcopy(
                    piece(chain, n), piece(chain, n), cd_s.at[chain, n], cd_r.at[chain, n], partner, c
                ).wait_send()

    @pl.when(row_src)
    def _():
        for d in range(1, 4):
            rcopy(ecol, erow.at[e], e1_s.at[d], e1_r.at[0], r, xcol(d)).wait_send()

    @pl.when(pan_src)
    def _():
        for d in range(1, 4):
            rcopy(ecol, epan, p1_s.at[d], p1_r.at[0], r, xcol(d)).wait_send()

    @pl.when(in_rows)
    def _():
        for d in range(1, 4):
            rcopy(erow.at[e], erow.at[e], e2_s.at[d], e2_r.at[e], r, ycol(d)).wait_send()

    @pl.when(y == 0)
    def _():
        for d in range(1, 4):
            rcopy(epan, epan, p2_s.at[d], p2_r.at[0], r, ycol(d)).wait_send()

    for copy in done:
        copy.wait()


def factors(act, erow, ecol, epan, capall, colp, r01, s0, l0, l0t, l1, l1t, growt, rhsg, rhsr, grow, gcol, gpan, gpt, w01, w01t):
    c = lax.axis_index("col")

    @pl.loop(0, 2)
    def _(h):
        for half in range(2):
            for idx in range(2):
                q = h * 4 + half * 2 + idx
                order = [(j % 4) * 4 + j // 4 if half == 0 else j for j in range(16)]
                right = jnp.concatenate([act[h, half, s, idx] for s in order], axis=0)
                ids = lax.broadcasted_iota(jnp.int32, (64, 1024), 0)
                member = (capall[q] == ids).astype(F32).astype(BF)
                spot = pl.ds(pl.multiple_of(q * 64, 64), 64)
                for src, dst, base in (
                    (erow.at[0], grow, 0), (erow.at[1], grow, 1024), (ecol, gcol, 0), (epan, gpan, 0),
                ):
                    e8 = src[q]
                    left = jnp.concatenate([member * e8[i : i + 1, :] for i in range(8)], axis=0)
                    out = dot(left, right).astype(BF)
                    for i in range(8):
                        dst[spot, base + i * 128 : base + (i + 1) * 128] = out[i * 64 : (i + 1) * 64]

    scale = 1.0 / 512.0
    for n in range(2):
        gpt[n * 512 : (n + 1) * 512, :] = gpan[:, n * 512 : (n + 1) * 512].T
    for n in range(4):
        growt[n * 512 : (n + 1) * 512, :] = grow[:, n * 512 : (n + 1) * 512].T
    a01 = (r01[...].astype(F32) + dot(gpt[0:512, :], gpan[:, 512:1024]) * scale).astype(BF)
    mixed = dot(s0[...], a01).astype(BF)
    corner = -dot(mixed, l1t[...])
    w01[...] = corner.astype(BF)
    w01t[...] = corner.T.astype(BF)

    @pl.when(c == 0)
    def _():
        rhsr[0:512, 0:512] = l0t[...]
        rhsr[0:512, 512:1024] = w01[...]
        rhsr[512:1024, 0:512] = jnp.zeros((512, 512), BF)
        rhsr[512:1024, 512:1024] = l1t[...]

    @pl.when(c != 0)
    def _():
        @pl.loop(0, 4)
        def _(n):
            part = pl.ds(pl.multiple_of(n * 256, 256), 256)
            at = (colp[:, part].astype(F32) + dot(gpt[...], gcol[:, part]) * scale).astype(BF)
            u0 = dot(l0[...], at[0:512]).astype(BF)
            u1 = (dot(w01t[...], at[0:512]) + dot(l1[...], at[512:1024])).astype(BF)
            rhsr[0:512, part] = (-(dot(l0t[...], u0) + dot(w01[...], u1))).astype(BF)
            rhsr[512:1024, part] = (-dot(l1t[...], u1)).astype(BF)

    @pl.loop(0, 4)
    def _(n):
        part = pl.ds(pl.multiple_of(n * 256, 256), 256)
        own = jnp.where(c == 0, 0.0, gcol[:, part].astype(F32))
        rhsg[:, part] = ((own + dot(gpan[...], rhsr[:, part])) * scale).astype(BF)


def finish(ridge, growt, rows, rhsg, rhsr, out):
    r = lax.axis_index("row")
    c = lax.axis_index("col")
    n = pl.program_id(0)
    height, width = out.shape
    value = dot(growt[...], rhsg[...]) + dot(rows[...], rhsr[...])
    value = value + jnp.where(c == 0, 0.0, ridge[...])
    row_ids = r * 2048 + n * height + lax.broadcasted_iota(jnp.int32, (height, width), 0)
    col_ids = c * 1024 + lax.broadcasted_iota(jnp.int32, (height, width), 1)
    above = jnp.logical_or(
        jnp.logical_and(row_ids < 512, col_ids >= 512), jnp.logical_and(row_ids < 1024, col_ids >= 1024)
    )
    out[...] = jnp.where(above, 0.0, value)


def shape(dims, kind):
    return jax.ShapeDtypeStruct(dims, kind)


VM = pl.BlockSpec(memory_space=pltpu.VMEM)
ANY = pl.BlockSpec(memory_space=pl.ANY)
DMA = pltpu.SemaphoreType.DMA


def per_device(activations, errors, act_proj, err_proj, lengths, ridge, pivot_inverse):
    pact = jnp.dot(activations, act_proj, preferred_element_type=F32).astype(BF).reshape(16, 64, 128)
    perr = lax.dot_general(
        err_proj, errors, (((0,), (1,)), ((), ())), preferred_element_type=F32
    ).astype(BF).reshape(16, 8, 1024)
    ends = jnp.cumsum(lengths[0])
    positions = jnp.arange(1024, dtype=jnp.int32)
    cap = jnp.sum((positions[None, :] >= ends[:, None]).astype(jnp.int32), axis=0).reshape(1, 1, 1024)

    moved = (
        ((2, 2, 16, 2, 64, 128), BF), ((2, 8, 8, 1024), BF), ((8, 8, 1024), BF), ((8, 8, 1024), BF),
        ((8, 1, 1024), jnp.int32), ((2048, 1024), BF), ((1024, 1024), BF), ((512, 512), BF),
    )
    act, erow, ecol, epan, capall, rows, colp, r01 = pl.pallas_call(
        exchange,
        out_shape=tuple(shape(*m) for m in moved),
        in_specs=[VM, VM, VM, ANY],
        out_specs=(ANY,) * 8,
        scratch_shapes=[pltpu.VMEM(*m) for m in moved]
        + [
            pltpu.VMEM((16, 64, 128), BF), pltpu.VMEM((16, 8, 1024), BF),
            pltpu.VMEM((64, 128), BF), pltpu.VMEM((8, 1024), BF), pltpu.VMEM((2048, 1024), F32),
        ]
        + [
            DMA((2, 16)), DMA((2, 16)), DMA((4,)), DMA((2, 2)), DMA((8,)), DMA((8,)), DMA((8,)), DMA((8,)),
            DMA((2, 4)), DMA((2, 4)), DMA((2, 4)), DMA((2, 4)), DMA((2, 4)), DMA((2, 4)), DMA((2, 4)), DMA((2, 4)),
            DMA((4,)), DMA((1,)), DMA((4,)), DMA((2,)), DMA((4,)), DMA((1,)), DMA((4,)), DMA((1,)), DMA, DMA,
            DMA((4, CH + 1)), DMA((4, CH + 1)), DMA((8,)), DMA((6,)), DMA((8,)),
        ],
        compiler_params=pltpu.CompilerParams(
            collective_id=0, has_side_effects=True, vmem_limit_bytes=VMEM_LIMIT
        ),
        name="exchange",
    )(pact, perr, cap, ridge)

    l0, l1 = pivot_inverse[0], pivot_inverse[1]
    s0 = lax.dot_general(l0, l0, (((0,), (0,)), ((), ())), precision=lax.Precision.HIGHEST).astype(BF)
    growt, rhsg, rhsr = pl.pallas_call(
        factors,
        out_shape=(shape((2048, 512), BF), shape((512, 1024), BF), shape((1024, 1024), BF)),
        in_specs=[VM] * 12,
        out_specs=(VM,) * 3,
        scratch_shapes=[
            pltpu.VMEM((512, 2048), BF), pltpu.VMEM((512, 1024), BF), pltpu.VMEM((512, 1024), BF),
            pltpu.VMEM((1024, 512), BF), pltpu.VMEM((512, 512), BF), pltpu.VMEM((512, 512), BF),
        ],
        compiler_params=pltpu.CompilerParams(vmem_limit_bytes=VMEM_LIMIT),
        name="factors",
    )(
        act, erow, ecol, epan, capall, colp, r01, s0,
        l0.astype(BF), l0.T.astype(BF), l1.astype(BF), l1.T.astype(BF),
    )

    step = 256
    return pl.pallas_call(
        finish,
        out_shape=shape((2048, 1024), F32),
        grid=(2048 // step,),
        in_specs=[
            pl.BlockSpec((step, 1024), lambda n: (n, 0)),
            pl.BlockSpec((step, 512), lambda n: (n, 0)),
            pl.BlockSpec((step, 1024), lambda n: (n, 0)),
            pl.BlockSpec((512, 1024), lambda n: (0, 0)),
            pl.BlockSpec((1024, 1024), lambda n: (0, 0)),
        ],
        out_specs=pl.BlockSpec((step, 1024), lambda n: (n, 0)),
        compiler_params=pltpu.CompilerParams(vmem_limit_bytes=VMEM_LIMIT),
        name="finish",
    )(ridge, growt, rows, rhsg, rhsr)


def solution(mesh):
    in_specs = (
        P("row", "col"), P("row", "col"), P("col", None), P("col", None),
        P("row", None), P("row", "col"), P(),
    )
    return jax.shard_map(
        per_device, mesh=mesh, in_specs=in_specs, out_specs=P("row", "col"), check_vma=False
    )
```

```python
import jax
import jax.numpy as jnp
from jax import lax
from jax.experimental import pallas as pl
from jax.experimental.pallas import tpu as pltpu
from jax.sharding import PartitionSpec as P

MESH = pl.DeviceIdType.MESH
BF = jnp.bfloat16
F32 = jnp.float32
CT = 18
Q01 = 13
VMEM_LIMIT = 66000000


def dot(a, b):
    return jnp.dot(a, b, preferred_element_type=F32)


def rcopy(src, dst, ssem, rsem, r, c):
    return pltpu.make_async_remote_copy(
        src_ref=src, dst_ref=dst, send_sem=ssem, recv_sem=rsem, device_id=(r, c), device_id_type=MESH
    )


def flip(v, bit):
    return v + 1 - 2 * (v % 2) if bit == 0 else 3 - v


def exchange(
    pact, perr, cap, piv, ridge,
    growt_o, rows_o, rhsg_o, rhsr_o,
    act, erow, ecol, epan, capall, big, colp, ra1, re1, sa1, se1, ra2, re2, my_act, my_err, stage,
    l0, l0t, l1, l1t, s0, grow, gcol, gpan, gpt, growt, r01, w01, w01t, rhsg, rhsr,
    r1_s, r1_r, r2_s, r2_r, sa_s, sa_r, se_s, se_r, cp_s, cp_r,
    cz_s, cz_r, cd_s, cd_r, b1_s, b1_r, b2_s, b2_r,
    e1_s, e1_r, e2_s, e2_r, p1_s, p1_r, p2_s, p2_r, d2_s, d2_r,
    ts, tr, ld, loc, outs,
):
    r = lax.axis_index("row")
    c = lax.axis_index("col")
    z, k = r // 2, r % 2
    x, y = c // 4, c % 4
    partner = 2 * z + 1 - k

    def row_of(dz, dk):
        return 2 * ((z + dz) % 4) + (k + dk) % 2

    def xcol(d):
        return 4 * ((x + d) % 4) + y

    def ycol(d):
        return 4 * x + (y + d) % 4

    column = [(dz, dk) for dz in range(4) for dk in range(2) if dz or dk]
    loads = [
        pltpu.make_async_copy(ridge.at[pl.ds(n * 256, 256)], stage.at[pl.ds(n * 256, 256)], ld.at[n])
        for n in range(8)
    ]

    @pl.when(jnp.logical_or(c == 0, r == 0))
    def _():
        for copy in loads:
            copy.start()

    barrier = pltpu.get_barrier_semaphore()
    for d in range(1, 16):
        pl.semaphore_signal(barrier, inc=1, device_id=(r, (c + d) % 16), device_id_type=MESH)
    for dz, dk in column:
        pl.semaphore_signal(barrier, inc=1, device_id=(row_of(dz, dk), c), device_id_type=MESH)
    pl.semaphore_wait(barrier, 22)

    sends = []

    def go(copy):
        copy.start()
        sends.append(copy)

    for d in range(1, 4):
        go(rcopy(pact.at[pl.ds(4 * ((y + d) % 4), 4)], ra1.at[d], r1_s.at[0, d], r1_r.at[0, d], r, ycol(d)))
        go(rcopy(perr.at[pl.ds(4 * ((x + d) % 4), 4)], re1.at[d], r1_s.at[1, d], r1_r.at[1, d], r, xcol(d)))
    for dz, dk in column:
        n = 2 * dz + dk
        go(rcopy(cap.at[0], capall.at[r], cp_s.at[n], cp_r.at[n], row_of(dz, dk), c))
    own_cap = pltpu.make_async_copy(cap.at[0], capall.at[r], loc.at[0])
    own_cap.start()

    @pl.when(jnp.logical_or(c == 0, r == 0))
    def _():
        for copy in loads:
            copy.wait()

    @pl.when(r == 0)
    def _():
        @pl.loop(0, 16)
        def _(n):
            part = pl.ds(pl.multiple_of(n * 64, 64), 64)
            colp[part, :] = stage[part, :].astype(BF)

    @pl.when(c == 0)
    def _():
        @pl.loop(0, 16)
        def _(n):
            q = n + jnp.where(n >= Q01, 2, 0)
            for t in range(4):
                big[t, q] = stage[pl.ds(pl.multiple_of(t * 512 + n * 32, 32), 32), :].astype(BF)

    def piece(chain, n):
        return colp.at[pl.ds(pl.multiple_of(chain * 512 + n * 128, 128), 128)]

    def place_of(chain):
        return z if chain == 0 else (4 - z) % 4

    def along(chain, n):
        follow = 2 * ((z + 1) % 4) if chain == 0 else 2 * ((z + 3) % 4)
        return rcopy(piece(chain, n), piece(chain, n), cz_s.at[chain, n], cz_r.at[chain, n], follow, c)

    def across(chain, n):
        return rcopy(piece(chain, n), piece(chain, n), cd_s.at[chain, n], cd_r.at[chain, n], partner, c)

    @pl.when(r == 0)
    def _():
        for n in range(4):
            for chain in range(2):
                along(chain, n).start()
                across(chain, n).start()

    def chain_round(j):
        for chain in range(2):
            place = place_of(chain)
            n = j - jnp.where(place == 2, 1, 0)
            inner = jnp.logical_or(place == 1, place == 2)
            on = jnp.logical_and(inner, jnp.logical_and(n >= 0, n < 4))

            @pl.when(jnp.logical_and(k == 0, on))
            def _():
                along(chain, n).wait_recv()
                along(chain, n).start()
                across(chain, n).start()

    def chain_ends():
        for n in range(4):
            for chain in range(2):

                @pl.when(jnp.logical_and(k == 0, place_of(chain) == 3))
                def _():
                    along(chain, n).wait_recv()
                    across(chain, n).start()

                @pl.when(k == 1)
                def _():
                    across(chain, n).wait_recv()

    bits = [((x + 1) // 2) % 2, ((y + 1) // 2) % 2, x // 2, y // 2]
    count = bits[0] + bits[1] + bits[2] + bits[3]
    nbr = [4 * flip(x, 0) + y, 4 * x + flip(y, 0), 4 * flip(x, 1) + y, 4 * x + flip(y, 1)]
    tree = []
    for d in range(4):
        d1, d2, d3 = (d + 1) % 4, (d + 2) % 4, (d + 3) % 4
        up = jnp.where(bits[d1] == 1, d1, jnp.where(bits[d2] == 1, d2, jnp.where(bits[d3] == 1, d3, d)))
        tree.append(jnp.where(bits[d] == 1, d, up))
    sends_on = [jnp.logical_or(bits[d] == 0, count > 1) for d in range(4)]

    def hop(t, q, d):
        return rcopy(big.at[t, q], big.at[t, q], ts.at[d, q], tr.at[t, q], r, nbr[d])

    def step(s):
        q = s - 2 * count

        @pl.when(jnp.logical_and(q >= 0, q < CT))
        def _():
            for t in range(4):

                @pl.when(bits[t] == 1)
                def _():
                    hop(t, q, 0).wait_recv()

            for d in range(4):

                @pl.when(sends_on[d])
                def _():
                    hop(tree[d], q, d).start()

    def leaves(q):
        for t in range(4):

            @pl.when(jnp.logical_and(bits[t] == 0, count > 0))
            def _():
                hop(t, q, 0).wait_recv()

        for d in range(4):

            @pl.when(sends_on[d])
            def _():
                hop(tree[d], q, d).wait_send()

    step(0)
    step(1)
    for src, plain, turned in ((piv.at[0], l0, l0t), (piv.at[1], l1, l1t)):
        plain[...] = src[...].astype(BF)
        turned[...] = src[...].T.astype(BF)

    step(2)
    for d in range(1, 4):
        rcopy(pact.at[pl.ds(0, 4)], ra1.at[d], r1_s.at[0, d], r1_r.at[0, d], partner, c).wait_recv()
    sa1[...] = pact[pl.ds(4 * y, 4)] + ra1[1] + ra1[2] + ra1[3]
    for d in range(1, 4):
        rcopy(perr.at[pl.ds(0, 4)], re1.at[d], r1_s.at[1, d], r1_r.at[1, d], partner, c).wait_recv()
    se1[...] = perr[pl.ds(4 * x, 4)] + re1[1] + re1[2] + re1[3]
    for d in range(1, 4):
        go(rcopy(sa1.at[(x + d) % 4], ra2.at[d], r2_s.at[0, d], r2_r.at[0, d], r, xcol(d)))
        go(rcopy(se1.at[(y + d) % 4], re2.at[d], r2_s.at[1, d], r2_r.at[1, d], r, ycol(d)))
    chain_round(0)
    step(3)
    s0[...] = dot(l0t[...], l0[...]).astype(BF)
    for d in range(1, 4):
        rcopy(sa1.at[0], ra2.at[d], r2_s.at[0, d], r2_r.at[0, d], partner, c).wait_recv()
        rcopy(se1.at[0], re2.at[d], r2_s.at[1, d], r2_r.at[1, d], partner, c).wait_recv()
    my_act[...] = (sa1[x] + ra2[1] + ra2[2] + ra2[3]).astype(BF)
    my_err[...] = (se1[y] + re2[1] + re2[2] + re2[3]).astype(BF)

    h, half = z // 2, z % 2
    slot = jnp.where(half == 0, 4 * y + x, c)
    mine = act.at[h, half, slot, k]
    own_act = pltpu.make_async_copy(my_act, mine, loc.at[1])
    own_err = pltpu.make_async_copy(my_err, ecol.at[r], loc.at[2])
    own_err.start()

    @pl.when(h == k)
    def _():
        own_act.start()

    @pl.when(h != k)
    def _():
        rcopy(my_act, mine, sa_s.at[0], sa_r.at[half, k], partner, c).start()

    for dz in range(1, 4):
        go(rcopy(my_act, mine, sa_s.at[dz], sa_r.at[half, k], 2 * ((z + dz) % 4) + h, c))
    for dz, dk in column:
        n = 2 * dz + dk
        go(rcopy(my_err, ecol.at[r], se_s.at[n], se_r.at[n], row_of(dz, dk), c))

    chain_round(1)
    step(4)
    step(5)

    for i in range(2):
        for j in range(2):
            away = jnp.logical_or(z != 2 * k + i, k != j)
            into = act.at[k, i, jnp.where(jnp.int32(i) == 0, 4 * y + x, c), j]

            @pl.when(away)
            def _():
                rcopy(my_act, into, sa_s.at[0], sa_r.at[i, j], partner, c).wait_recv()

    @pl.when(h == k)
    def _():
        own_act.wait()

    slot0, slot1 = 4 * y + x, c
    for d in range(1, 4):
        go(rcopy(act.at[k, 0, slot0], act.at[k, 0, slot0], b1_s.at[0, d], b1_r.at[0, d], r, xcol(d)))
        go(rcopy(act.at[k, 1, slot1], act.at[k, 1, slot1], b1_s.at[1, d], b1_r.at[1, d], r, ycol(d)))

    own_err.wait()
    for dz, dk in column:
        n = 2 * dz + dk
        rcopy(my_err, ecol.at[row_of(4 - dz, 2 - dk)], se_s.at[n], se_r.at[n], partner, c).wait_recv()

    in_rows = y // 2 == k
    e = y % 2
    row_src = jnp.logical_and(in_rows, x == z)
    pan_src = c == 0

    @pl.when(row_src)
    def _():
        for d in range(1, 4):
            rcopy(ecol, erow.at[e], e1_s.at[d], e1_r.at[0], r, xcol(d)).start()
        copy = pltpu.make_async_copy(ecol, erow.at[e], loc.at[3])
        copy.start()
        copy.wait()

    @pl.when(pan_src)
    def _():
        for d in range(1, 4):
            rcopy(ecol, epan, p1_s.at[d], p1_r.at[0], r, xcol(d)).start()
        copy = pltpu.make_async_copy(ecol, epan, loc.at[4])
        copy.start()
        copy.wait()

    chain_round(2)
    step(6)
    step(7)

    @pl.when(jnp.logical_and(in_rows, x != z))
    def _():
        rcopy(ecol, erow.at[e], e1_s.at[0], e1_r.at[0], r, xcol(1)).wait_recv()

    @pl.when(in_rows)
    def _():
        for d in range(1, 4):
            rcopy(erow.at[e], erow.at[e], e2_s.at[d], e2_r.at[e], r, ycol(d)).start()

    @pl.when(jnp.logical_and(y == 0, x != 0))
    def _():
        rcopy(ecol, epan, p1_s.at[0], p1_r.at[0], r, xcol(1)).wait_recv()

    @pl.when(y == 0)
    def _():
        for d in range(1, 4):
            rcopy(epan, epan, p2_s.at[d], p2_r.at[0], r, ycol(d)).start()

    for d in range(1, 4):
        from_x = 4 * y + (x + 4 - d) % 4
        from_y = 4 * x + (y + 4 - d) % 4
        rcopy(act.at[k, 0, slot0], act.at[k, 0, from_x], b1_s.at[0, d], b1_r.at[0, d], r, xcol(d)).wait_recv()
        rcopy(act.at[k, 1, slot1], act.at[k, 1, from_y], b1_s.at[1, d], b1_r.at[1, d], r, ycol(d)).wait_recv()
    g0, g1 = pl.ds(4 * y, 4), pl.ds(4 * x, 4)
    for d in range(1, 4):
        go(rcopy(act.at[k, 0, g0], act.at[k, 0, g0], b2_s.at[0, d], b2_r.at[0, d], r, ycol(d)))
        go(rcopy(act.at[k, 1, g1], act.at[k, 1, g1], b2_s.at[1, d], b2_r.at[1, d], r, xcol(d)))

    chain_round(3)
    step(8)
    step(9)
    step(10)
    chain_round(4)
    step(11)
    step(12)

    for d in range(1, 4):
        far0 = pl.ds(4 * ((y + 4 - d) % 4), 4)
        far1 = pl.ds(4 * ((x + 4 - d) % 4), 4)
        rcopy(act.at[k, 0, g0], act.at[k, 0, far0], b2_s.at[0, d], b2_r.at[0, d], r, ycol(d)).wait_recv()
        rcopy(act.at[k, 1, g1], act.at[k, 1, far1], b2_s.at[1, d], b2_r.at[1, d], r, xcol(d)).wait_recv()
    go(rcopy(act.at[k], act.at[k], d2_s, d2_r, partner, c))
    chain_ends()

    @pl.when(c == 0)
    def _():
        for t in range(4):
            for u in range(2):
                for b in range(2):
                    at = 256 * b + 64 * t + 32 * u
                    big[t, Q01 + u, :, b * 512 : (b + 1) * 512] = colp[at : at + 32, 512:1024]

    for i in range(2):

        @pl.when(y != 2 * k + i)
        def _():
            rcopy(erow.at[i], erow.at[i], e2_s.at[0], e2_r.at[i], r, ycol(1)).wait_recv()

    @pl.when(y != 0)
    def _():
        rcopy(epan, epan, p2_s.at[0], p2_r.at[0], r, ycol(1)).wait_recv()

    own_cap.wait()
    for dz, dk in column:
        n = 2 * dz + dk
        rcopy(cap.at[0], capall.at[row_of(4 - dz, 2 - dk)], cp_s.at[n], cp_r.at[n], partner, c).wait_recv()

    def gradients(h, half, idx):
        q = h * 4 + half * 2 + idx
        order = [(j % 4) * 4 + j // 4 if half == 1 else j for j in range(16)]
        right = jnp.concatenate([act[h, half, s, idx] for s in order], axis=0)
        ids = lax.broadcasted_iota(jnp.int32, (64, 1024), 0)
        member = (capall[q] == ids).astype(F32).astype(BF)
        spot = pl.ds(pl.multiple_of(q * 64, 64), 64)
        for src, dst, base in (
            (erow.at[0], grow, 0), (erow.at[1], grow, 1024), (ecol, gcol, 0), (epan, gpan, 0),
        ):
            e8 = src[q]
            left = jnp.concatenate([member * e8[i : i + 1, :] for i in range(8)], axis=0)
            out = dot(left, right).astype(BF)
            for i in range(8):
                dst[spot, base + i * 128 : base + (i + 1) * 128] = out[i * 64 : (i + 1) * 64]

    step(13)

    @pl.loop(0, 2)
    def _(i):
        @pl.when(i == 1)
        def _():
            rcopy(act.at[k], act.at[1 - k], d2_s, d2_r, partner, c).wait_recv()

        for n in range(4):
            gradients((k + i) % 2, n // 2, n % 2)
            step(14 + 4 * i + n)

    scale = 1.0 / 512.0
    for n in range(2):
        gpt[n * 512 : (n + 1) * 512, :] = gpan[:, n * 512 : (n + 1) * 512].T
    step(22)
    for n in range(4):
        growt[n * 512 : (n + 1) * 512, :] = grow[:, n * 512 : (n + 1) * 512].T
    out_growt = pltpu.make_async_copy(growt, growt_o, outs.at[0])
    out_growt.start()
    step(23)

    def ends(q):
        for t in range(4):

            @pl.when(jnp.logical_and(bits[t] == 0, count > 0))
            def _():
                hop(t, q, 0).wait_recv()

    @pl.loop(24, Q01 + 10)
    def _(s):
        step(s)

    for u in range(2):
        ends(Q01 + u)
    for t in range(4):
        for u in range(2):
            for b in range(2):
                at = 256 * b + 64 * t + 32 * u
                r01[at : at + 32, :] = big[t, Q01 + u, :, b * 512 : (b + 1) * 512]
    a01 = (r01[...].astype(F32) + dot(gpt[0:512, :], gpan[:, 512:1024]) * scale).astype(BF)
    corner = -dot(dot(s0[...], a01).astype(BF), l1t[...])
    w01[...] = corner.astype(BF)
    w01t[...] = corner.T.astype(BF)

    @pl.when(c == 0)
    def _():
        rhsr[0:512, 0:512] = l0t[...]
        rhsr[0:512, 512:1024] = w01[...]
        rhsr[512:1024, 0:512] = jnp.zeros((512, 512), BF)
        rhsr[512:1024, 512:1024] = l1t[...]

    late = max(24, Q01 + 10)

    @pl.loop(0, 4)
    def _(n):
        part = pl.ds(pl.multiple_of(n * 256, 256), 256)

        @pl.when(c != 0)
        def _():
            at = (colp[:, part].astype(F32) + dot(gpt[...], gcol[:, part]) * scale).astype(BF)
            u0 = dot(l0[...], at[0:512]).astype(BF)
            u1 = (dot(w01t[...], at[0:512]) + dot(l1[...], at[512:1024])).astype(BF)
            rhsr[0:512, part] = (-(dot(l0t[...], u0) + dot(w01[...], u1))).astype(BF)
            rhsr[512:1024, part] = (-dot(l1t[...], u1)).astype(BF)

        own = jnp.where(c == 0, 0.0, gcol[:, part].astype(F32))
        rhsg[:, part] = ((own + dot(gpan[...], rhsr[:, part])) * scale).astype(BF)
        step(late + n)

    out_rhs = [pltpu.make_async_copy(rhsg, rhsg_o, outs.at[1]), pltpu.make_async_copy(rhsr, rhsr_o, outs.at[2])]
    for copy in out_rhs:
        copy.start()

    @pl.loop(late + 4, CT + 8)
    def _(s):
        step(s)

    for t in range(4):

        @pl.when(jnp.logical_or(bits[t] == 1, count == 0))
        def _():
            for q in range(16):
                src = q + (2 if q >= Q01 else 0)
                pltpu.make_async_copy(
                    big.at[t, src], rows_o.at[pl.ds(t * 512 + q * 32, 32)], ld.at[t]
                ).start()

    @pl.loop(0, CT)
    def _(q):
        for t in range(4):

            @pl.when(jnp.logical_and(bits[t] == 0, count > 0))
            def _():
                @pl.when(jnp.logical_or(q < Q01, q >= Q01 + 2))
                def _():
                    hop(t, q, 0).wait_recv()
                    at = 512 * t + 32 * (q - jnp.where(q >= Q01, 2, 0))
                    pltpu.make_async_copy(
                        big.at[t, q], rows_o.at[pl.ds(pl.multiple_of(at, 32), 32)], ld.at[t]
                    ).start()

        for d in range(4):

            @pl.when(sends_on[d])
            def _():
                hop(tree[d], q, d).wait_send()

    out_growt.wait()
    for copy in out_rhs:
        copy.wait()
    for t in range(4):
        whole = rows_o.at[pl.ds(t * 512, 512)]
        pltpu.make_async_copy(whole, whole, ld.at[t]).wait()

    for copy in sends:
        copy.wait_send()

    @pl.when(h != k)
    def _():
        rcopy(my_act, mine, sa_s.at[0], sa_r.at[half, k], partner, c).wait_send()

    @pl.when(k == 0)
    def _():
        for n in range(4):
            for chain in range(2):

                @pl.when(place_of(chain) < 3)
                def _():
                    along(chain, n).wait_send()

                across(chain, n).wait_send()

    @pl.when(row_src)
    def _():
        for d in range(1, 4):
            rcopy(ecol, erow.at[e], e1_s.at[d], e1_r.at[0], r, xcol(d)).wait_send()

    @pl.when(pan_src)
    def _():
        for d in range(1, 4):
            rcopy(ecol, epan, p1_s.at[d], p1_r.at[0], r, xcol(d)).wait_send()

    @pl.when(in_rows)
    def _():
        for d in range(1, 4):
            rcopy(erow.at[e], erow.at[e], e2_s.at[d], e2_r.at[e], r, ycol(d)).wait_send()

    @pl.when(y == 0)
    def _():
        for d in range(1, 4):
            rcopy(epan, epan, p2_s.at[d], p2_r.at[0], r, ycol(d)).wait_send()


def finish(ridge, growt, rows, rhsg, rhsr, out):
    r = lax.axis_index("row")
    c = lax.axis_index("col")
    n = pl.program_id(0)
    height, width = out.shape
    value = dot(growt[...], rhsg[...]) + dot(rows[...], rhsr[...])
    value = value + jnp.where(c == 0, 0.0, ridge[...])
    row_ids = r * 2048 + n * height + lax.broadcasted_iota(jnp.int32, (height, width), 0)
    col_ids = c * 1024 + lax.broadcasted_iota(jnp.int32, (height, width), 1)
    above = jnp.logical_or(
        jnp.logical_and(row_ids < 512, col_ids >= 512), jnp.logical_and(row_ids < 1024, col_ids >= 1024)
    )
    out[...] = jnp.where(above, 0.0, value)


def shape(dims, kind):
    return jax.ShapeDtypeStruct(dims, kind)


VM = pl.BlockSpec(memory_space=pltpu.VMEM)
ANY = pl.BlockSpec(memory_space=pl.ANY)
DMA = pltpu.SemaphoreType.DMA


def per_device(activations, errors, act_proj, err_proj, lengths, ridge, pivot_inverse):
    pact = jnp.dot(activations, act_proj, preferred_element_type=F32).reshape(16, 64, 128)
    perr = lax.dot_general(
        err_proj, errors, (((0,), (1,)), ((), ())), preferred_element_type=F32
    ).reshape(16, 8, 1024)
    ends = jnp.cumsum(lengths[0])
    positions = jnp.arange(1024, dtype=jnp.int32)
    cap = jnp.sum((positions[None, :] >= ends[:, None]).astype(jnp.int32), axis=0).reshape(1, 1, 1024)

    growt, rows, rhsg, rhsr = pl.pallas_call(
        exchange,
        out_shape=(
            shape((2048, 512), BF), shape((2048, 1024), BF), shape((512, 1024), BF), shape((1024, 1024), BF)
        ),
        in_specs=[VM, VM, VM, VM, ANY],
        out_specs=(ANY,) * 4,
        scratch_shapes=[
            pltpu.VMEM((2, 2, 16, 2, 64, 128), BF), pltpu.VMEM((2, 8, 8, 1024), BF),
            pltpu.VMEM((8, 8, 1024), BF), pltpu.VMEM((8, 8, 1024), BF), pltpu.VMEM((8, 1, 1024), jnp.int32),
            pltpu.VMEM((4, CT, 32, 1024), BF), pltpu.VMEM((1024, 1024), BF),
            pltpu.VMEM((4, 4, 64, 128), F32), pltpu.VMEM((4, 4, 8, 1024), F32),
            pltpu.VMEM((4, 64, 128), F32), pltpu.VMEM((4, 8, 1024), F32),
            pltpu.VMEM((4, 64, 128), F32), pltpu.VMEM((4, 8, 1024), F32),
            pltpu.VMEM((64, 128), BF), pltpu.VMEM((8, 1024), BF), pltpu.VMEM((2048, 1024), F32),
        ]
        + [pltpu.VMEM((512, 512), BF)] * 5
        + [
            pltpu.VMEM((512, 2048), BF), pltpu.VMEM((512, 1024), BF), pltpu.VMEM((512, 1024), BF),
            pltpu.VMEM((1024, 512), BF), pltpu.VMEM((2048, 512), BF),
        ]
        + [pltpu.VMEM((512, 512), BF)] * 3
        + [pltpu.VMEM((512, 1024), BF), pltpu.VMEM((1024, 1024), BF)]
        + [
            DMA((2, 4)), DMA((2, 4)), DMA((2, 4)), DMA((2, 4)),
            DMA((4,)), DMA((2, 2)), DMA((8,)), DMA((8,)), DMA((8,)), DMA((8,)),
            DMA((2, 4)), DMA((2, 4)), DMA((2, 4)), DMA((2, 4)), DMA((2, 4)), DMA((2, 4)), DMA((2, 4)), DMA((2, 4)),
            DMA((4,)), DMA((1,)), DMA((4,)), DMA((2,)), DMA((4,)), DMA((1,)), DMA((4,)), DMA((1,)), DMA, DMA,
            DMA((4, CT)), DMA((4, CT)), DMA((8,)), DMA((6,)), DMA((4,)),
        ],
        compiler_params=pltpu.CompilerParams(
            collective_id=0, has_side_effects=True, vmem_limit_bytes=VMEM_LIMIT
        ),
        name="exchange",
    )(pact, perr, cap, pivot_inverse, ridge)

    step = 512
    return pl.pallas_call(
        finish,
        out_shape=shape((2048, 1024), F32),
        grid=(2048 // step,),
        in_specs=[
            pl.BlockSpec((step, 1024), lambda n: (n, 0)),
            pl.BlockSpec((step, 512), lambda n: (n, 0)),
            pl.BlockSpec((step, 1024), lambda n: (n, 0)),
            pl.BlockSpec((512, 1024), lambda n: (0, 0)),
            pl.BlockSpec((1024, 1024), lambda n: (0, 0)),
        ],
        out_specs=pl.BlockSpec((step, 1024), lambda n: (n, 0)),
        compiler_params=pltpu.CompilerParams(vmem_limit_bytes=VMEM_LIMIT),
        name="finish",
    )(ridge, growt, rows, rhsg, rhsr)


def solution(mesh):
    in_specs = (
        P("row", "col"), P("row", "col"), P("col", None), P("col", None),
        P("row", None), P("row", "col"), P(),
    )
    return jax.shard_map(
        per_device, mesh=mesh, in_specs=in_specs, out_specs=P("row", "col"), check_vma=False
    )
```

```python
import jax
import jax.numpy as jnp
from jax import lax
from jax.experimental import pallas as pl
from jax.experimental.pallas import tpu as pltpu
from jax.sharding import PartitionSpec as P

MESH = pl.DeviceIdType.MESH
BF = jnp.bfloat16
F32 = jnp.float32
CT = 18
Q01 = 12
VMEM_LIMIT = 66000000


def dot(a, b):
    return jnp.dot(a, b, preferred_element_type=F32)


def rcopy(src, dst, ssem, rsem, r, c):
    return pltpu.make_async_remote_copy(
        src_ref=src, dst_ref=dst, send_sem=ssem, recv_sem=rsem, device_id=(r, c), device_id_type=MESH
    )


def flip(v, bit):
    return v + 1 - 2 * (v % 2) if bit == 0 else 3 - v


def gray(v):
    return [((v + 1) // 2) % 2, v // 2]


def order_of(t, c):
    (x0, x1), (y0, y1) = gray(c // 4), gray(c % 4)
    bits = [x0, y0, x1, y1]
    return sum(bits[(t + n) % 4] * (8 >> n) for n in range(4))


def trees_of(bits):
    count = bits[0] + bits[1] + bits[2] + bits[3]
    tree = []
    for d in range(4):
        d1, d2, d3 = (d + 1) % 4, (d + 2) % 4, (d + 3) % 4
        up = jnp.where(bits[d1] == 1, d1, jnp.where(bits[d2] == 1, d2, jnp.where(bits[d3] == 1, d3, d)))
        tree.append(jnp.where(bits[d] == 1, d, up))
    return tree, [jnp.logical_or(bits[d] == 0, count > 1) for d in range(4)]


def exchange(
    acts, errs, actp, errp, lens, piv_in, ridge,
    growt_o, rows_o, rhsg_o, rhsr_o,
    av, ev, piv, stage, part, in0, in1, in2, in3, my_act, my_err, near, act, erow, ecol, epan, cap, capall, big, colp,
    l0, l0t, l1, l1t, s0, grow, gcol, gpan, gpt, growt, atb, u0b, u1p, q0p, r01, w01, w01t, rhsg, rhsr,
    rs_s, rs_r, ag_s, ag_r, sa_s, sa_r, se_s, se_r, cp_s, cp_r,
    cz_s, cz_r, cd_s, cd_r,
    sp_s, sp_r, d2_s, d2_r,
    ts, tr, ld, loc, outs,
):
    r = lax.axis_index("row")
    c = lax.axis_index("col")
    z, k = r // 2, r % 2
    x, y = c // 4, c % 4
    partner = 2 * z + 1 - k

    get_act = pltpu.make_async_copy(acts, av, loc.at[0])
    get_err = pltpu.make_async_copy(errs, ev, loc.at[1])
    get_piv = pltpu.make_async_copy(piv_in, piv, loc.at[2])
    get_act.start()
    get_err.start()
    get_piv.start()

    def row_of(dz, dk):
        return 2 * ((z + dz) % 4) + (k + dk) % 2

    def xcol(d):
        return 4 * ((x + d) % 4) + y

    def ycol(d):
        return 4 * x + (y + d) % 4

    column = [(dz, dk) for dz in range(4) for dk in range(2) if dz or dk]
    loads = [
        pltpu.make_async_copy(ridge.at[pl.ds(n * 256, 256)], stage.at[pl.ds(n * 256, 256)], ld.at[n])
        for n in range(8)
    ]

    @pl.when(jnp.logical_or(c == 0, r == 0))
    def _():
        for copy in loads:
            copy.start()

    bits = [gray(x)[0], gray(y)[0], gray(x)[1], gray(y)[1]]
    count = bits[0] + bits[1] + bits[2] + bits[3]
    nbr = [4 * flip(x, 0) + y, 4 * x + flip(y, 0), 4 * flip(x, 1) + y, 4 * x + flip(y, 1)]

    barrier = pltpu.get_barrier_semaphore()
    for d in range(1, 16):
        pl.semaphore_signal(barrier, inc=1, device_id=(r, (c + d) % 16), device_id_type=MESH)
    for dz, dk in column:
        pl.semaphore_signal(barrier, inc=1, device_id=(row_of(dz, dk), c), device_id_type=MESH)

    get_act.wait()
    part[:, :, 0:16, :] = dot(av[...], actp[...]).reshape(4, 16, 16, 128)
    get_err.wait()
    turned_proj = errp[...].T
    for t in range(4):
        out = lax.dot_general(
            turned_proj, ev[t * 256 : (t + 1) * 256, :], (((1,), (1,)), ((), ())), preferred_element_type=F32
        )
        for n in range(16):
            part[t, order_of(t, n), 16:24, :] = out[8 * n : 8 * n + 8, 0:128]
            part[t, order_of(t, n), 24:32, :] = out[8 * n : 8 * n + 8, 128:256]

    lower = lax.broadcasted_iota(jnp.int32, (64, 64), 1) <= lax.broadcasted_iota(jnp.int32, (64, 64), 0)
    ends = jnp.sum(jnp.where(lower, lens[...].astype(F32), 0.0), axis=1, keepdims=True)
    past = lax.broadcasted_iota(jnp.int32, (64, 1024), 1).astype(F32) >= ends
    cap[0] = jnp.sum(past.astype(F32), axis=0, keepdims=True).astype(jnp.int32)

    pl.semaphore_wait(barrier, 22)

    sends = []

    def go(copy):
        copy.start()
        sends.append(copy)

    landing = [in0, in1, in2, in3]
    base = [[jnp.int32(0)] * 4]
    for n in range(4):
        base.append([base[n][t] + bits[(t + n) % 4] * (8 >> n) for t in range(4)])

    def halve(n, t):
        d, size = (t + n) % 4, 8 >> n
        away = base[n][t] + (1 - bits[d]) * size
        return rcopy(
            part.at[t, pl.ds(away, size)], landing[n].at[t], rs_s.at[n, t], rs_r.at[n, t], r, nbr[d]
        )

    def send_halves(n):
        for t in range(4):
            go(halve(n, t))

    def add_halves(n):
        size = 8 >> n
        for t in range(4):
            halve(n, t).wait_recv()
            keep = pl.ds(base[n + 1][t], size)
            part[t, keep] = part[t, keep] + landing[n][t]

    send_halves(0)
    for dz, dk in column:
        n = 2 * dz + dk
        go(rcopy(cap.at[0], capall.at[r], cp_s.at[n], cp_r.at[n], row_of(dz, dk), c))
    own_cap = pltpu.make_async_copy(cap.at[0], capall.at[r], loc.at[0])
    own_cap.start()

    @pl.when(jnp.logical_or(c == 0, r == 0))
    def _():
        for copy in loads:
            copy.wait()

    @pl.when(r == 0)
    def _():
        @pl.loop(0, 16)
        def _(n):
            some = pl.ds(pl.multiple_of(n * 64, 64), 64)
            colp[some, :] = stage[some, :].astype(BF)

    @pl.when(c == 0)
    def _():
        @pl.loop(0, 16)
        def _(n):
            q = n + jnp.where(n >= Q01, 2, 0)
            for t in range(4):
                big[t, q] = stage[pl.ds(pl.multiple_of(t * 512 + n * 32, 32), 32), :].astype(BF)

    def piece(chain, n):
        return colp.at[pl.ds(pl.multiple_of(chain * 512 + n * 128, 128), 128)]

    def place_of(chain):
        return z if chain == 0 else (4 - z) % 4

    def along(chain, n):
        follow = 2 * ((z + 1) % 4) if chain == 0 else 2 * ((z + 3) % 4)
        return rcopy(piece(chain, n), piece(chain, n), cz_s.at[chain, n], cz_r.at[chain, n], follow, c)

    def across(chain, n):
        return rcopy(piece(chain, n), piece(chain, n), cd_s.at[chain, n], cd_r.at[chain, n], partner, c)

    @pl.when(r == 0)
    def _():
        for n in range(4):
            for chain in range(2):
                along(chain, n).start()
                across(chain, n).start()

    def chain_round(j):
        for chain in range(2):
            place = place_of(chain)
            n = j - jnp.where(place == 2, 2, 0)
            inner = jnp.logical_or(place == 1, place == 2)
            on = jnp.logical_and(inner, jnp.logical_and(n >= 0, n < 4))

            @pl.when(jnp.logical_and(k == 0, on))
            def _():
                along(chain, n).wait_recv()
                along(chain, n).start()
                across(chain, n).start()

    def chain_ends():
        for n in range(4):
            for chain in range(2):

                @pl.when(jnp.logical_and(k == 0, place_of(chain) == 3))
                def _():
                    along(chain, n).wait_recv()
                    across(chain, n).start()

                @pl.when(k == 1)
                def _():
                    across(chain, n).wait_recv()

    tree, sends_on = trees_of(bits)

    def hop(t, q, d):
        return rcopy(big.at[t, q], big.at[t, q], ts.at[d, q], tr.at[t, q], r, nbr[d])

    def step(s):
        q = s - 2 * count

        @pl.when(jnp.logical_and(q >= 0, q < CT))
        def _():
            for t in range(4):

                @pl.when(bits[t] == 1)
                def _():
                    hop(t, q, 0).wait_recv()

            for d in range(4):

                @pl.when(sends_on[d])
                def _():
                    hop(tree[d], q, d).start()

    step(0)
    step(1)
    get_piv.wait()
    for src, plain, turned in ((piv.at[0], l0, l0t), (piv.at[1], l1, l1t)):
        plain[...] = src[...].astype(BF)
        turned[...] = src[...].T.astype(BF)
    s0[...] = dot(l0t[...], l0[...]).astype(BF)

    add_halves(0)
    send_halves(1)
    chain_round(0)
    step(2)
    add_halves(1)
    send_halves(2)
    chain_round(1)
    step(3)
    add_halves(2)
    send_halves(3)
    chain_round(2)
    step(4)
    add_halves(3)
    for t in range(4):
        block = part[t, base[4][t]].astype(BF)
        my_act[t] = block[0:16]
        my_err[:, t * 256 : t * 256 + 128] = part[t, base[4][t], 16:24, :].astype(BF)
        my_err[:, t * 256 + 128 : t * 256 + 256] = part[t, base[4][t], 24:32, :].astype(BF)

    h, half = z // 2, z % 2
    mine = near.at[half, k]
    own_act = pltpu.make_async_copy(my_act, mine, loc.at[1])
    own_err = pltpu.make_async_copy(my_err, ecol.at[r], loc.at[2])
    own_err.start()

    @pl.when(h == k)
    def _():
        own_act.start()

    @pl.when(h != k)
    def _():
        rcopy(my_act, mine, sa_s.at[0], sa_r.at[half, k], partner, c).start()

    for dz in range(1, 4):
        go(rcopy(my_act, mine, sa_s.at[dz], sa_r.at[half, k], 2 * ((z + dz) % 4) + h, c))
    for dz, dk in column:
        n = 2 * dz + dk
        go(rcopy(my_err, ecol.at[r], se_s.at[n], se_r.at[n], row_of(dz, dk), c))

    chain_round(3)
    step(5)
    step(6)

    for i in range(2):
        for j in range(2):
            away = jnp.logical_or(z != 2 * k + i, k != j)

            @pl.when(away)
            def _():
                rcopy(my_act, near.at[i, j], sa_s.at[0], sa_r.at[i, j], partner, c).wait_recv()

    @pl.when(h == k)
    def _():
        own_act.wait()

    for t in range(4):
        for i in range(2):
            for j in range(2):
                act[k, t, base[4][t], 2 * i + j] = near[i, j, t]

    def double(n, t):
        d, size = (t + n) % 4, 8 >> n
        held = act.at[k, t, pl.ds(base[n + 1][t], size)]
        return rcopy(held, held, ag_s.at[n, t], ag_r.at[n, t], r, nbr[d])

    def send_doubles(n):
        for t in range(4):
            go(double(n, t))

    def wait_doubles(n):
        size = 8 >> n
        for t in range(4):
            other = base[n][t] + (1 - bits[(t + n) % 4]) * size
            held = act.at[k, t, pl.ds(other, size)]
            rcopy(held, held, ag_s.at[n, t], ag_r.at[n, t], r, nbr[0]).wait_recv()

    send_doubles(3)
    own_err.wait()
    for dz, dk in column:
        n = 2 * dz + dk
        rcopy(my_err, ecol.at[row_of(4 - dz, 2 - dk)], se_s.at[n], se_r.at[n], partner, c).wait_recv()

    def spread(m, buf, from_x, from_y):
        root = [gray(from_x)[0], gray(from_y)[0], gray(from_x)[1], gray(from_y)[1]]
        rel = [bits[d] + root[d] - 2 * bits[d] * root[d] for d in range(4)]
        far = rel[0] + rel[1] + rel[2] + rel[3]
        which, on = trees_of(rel)

        def send(t, d):
            quarter = buf.at[pl.ds(2 * t, 2)]
            return rcopy(quarter, quarter, sp_s.at[m, d], sp_r.at[m, t], r, nbr[d])

        def relay(depth):
            @pl.when(far == depth)
            def _():
                if depth == 0:
                    copy = pltpu.make_async_copy(ecol, buf, loc.at[3])
                    copy.start()
                    copy.wait()
                for t in range(4):
                    if depth:

                        @pl.when(rel[t] == 1)
                        def _():
                            send(t, 0).wait_recv()

                for d in range(4):

                    @pl.when(on[d])
                    def _():
                        send(which[d], d).start()

        def finish():
            for t in range(4):

                @pl.when(jnp.logical_and(rel[t] == 0, far > 0))
                def _():
                    send(t, 0).wait_recv()

        def drain():
            for d in range(4):

                @pl.when(on[d])
                def _():
                    send(which[d], d).wait_send()

        return relay, finish, drain

    spreads = [
        spread(0, erow.at[0], z, 2 * k), spread(1, erow.at[1], z, 2 * k + 1),
        spread(2, epan, jnp.int32(0), jnp.int32(0)),
    ]

    def relay_all(depth):
        for relay, _, _ in spreads:
            relay(depth)

    relay_all(0)
    chain_round(4)
    step(7)
    wait_doubles(3)
    send_doubles(2)
    relay_all(1)
    chain_round(5)
    step(8)

    wait_doubles(2)
    send_doubles(1)
    relay_all(2)
    step(9)
    wait_doubles(1)
    send_doubles(0)
    relay_all(3)
    step(10)
    chain_ends()

    @pl.when(c == 0)
    def _():
        for t in range(4):
            for u in range(2):
                for b in range(2):
                    at = 256 * b + 64 * t + 32 * u
                    big[t, Q01 + u, :, b * 512 : (b + 1) * 512] = colp[at : at + 32, 512:1024]

    step(11)
    wait_doubles(0)
    go(rcopy(act.at[k], act.at[k], d2_s, d2_r, partner, c))

    relay_all(4)
    for _, finish_spread, _ in spreads:
        finish_spread()

    own_cap.wait()
    for dz, dk in column:
        n = 2 * dz + dk
        rcopy(cap.at[0], capall.at[row_of(4 - dz, 2 - dk)], cp_s.at[n], cp_r.at[n], partner, c).wait_recv()

    def gradients(h, n):
        q = h * 4 + n
        right = jnp.concatenate([act[h, t, :, n].reshape(256, 128) for t in range(4)], axis=0)
        ids = lax.broadcasted_iota(jnp.int32, (64, 1024), 0)
        member = (capall[q] == ids).astype(F32).astype(BF)
        spot = pl.ds(pl.multiple_of(q * 64, 64), 64)
        for src, dst, base in (
            (erow.at[0], grow, 0), (erow.at[1], grow, 1024), (ecol, gcol, 0), (epan, gpan, 0),
        ):
            e8 = src[q]
            left = jnp.concatenate([member * e8[i : i + 1, :] for i in range(8)], axis=0)
            out = dot(left, right).astype(BF)
            for i in range(8):
                dst[spot, base + i * 128 : base + (i + 1) * 128] = out[i * 64 : (i + 1) * 64]

    @pl.loop(0, 2)
    def _(i):
        @pl.when(i == 1)
        def _():
            rcopy(act.at[k], act.at[1 - k], d2_s, d2_r, partner, c).wait_recv()

        for n in range(4):
            gradients((k + i) % 2, n)
            step(12 + 4 * i + n)

    scale = 1.0 / 512.0
    for n in range(2):
        gpt[n * 512 : (n + 1) * 512, :] = gpan[:, n * 512 : (n + 1) * 512].T
    step(20)
    step(21)
    for n in range(4):
        growt[n * 512 : (n + 1) * 512, :] = grow[:, n * 512 : (n + 1) * 512].T
    out_growt = pltpu.make_async_copy(growt, growt_o, outs.at[0])
    out_growt.start()

    @pl.loop(0, 4)
    def _(n):
        cols = pl.ds(pl.multiple_of(n * 256, 256), 256)

        @pl.when(c != 0)
        def _():
            at = (colp[:, cols].astype(F32) + dot(gpt[...], gcol[:, cols]) * scale).astype(BF)
            atb[:, cols] = at
            u0 = dot(l0[...], at[0:512]).astype(BF)
            u1p[:, cols] = dot(l1[...], at[512:1024])
            q0p[:, cols] = dot(l0t[...], u0)

        step(22 + n)

    for u in range(2):
        for t in range(4):

            @pl.when(jnp.logical_and(bits[t] == 0, count > 0))
            def _():
                hop(t, Q01 + u, 0).wait_recv()

    for t in range(4):
        for u in range(2):
            for b in range(2):
                at = 256 * b + 64 * t + 32 * u
                r01[at : at + 32, :] = big[t, Q01 + u, :, b * 512 : (b + 1) * 512]
    a01 = (r01[...].astype(F32) + dot(gpt[0:512, :], gpan[:, 512:1024]) * scale).astype(BF)
    corner = -dot(dot(s0[...], a01).astype(BF), l1t[...])
    w01[...] = corner.astype(BF)
    w01t[...] = corner.T.astype(BF)

    @pl.when(c == 0)
    def _():
        rhsr[0:512, 0:512] = l0t[...]
        rhsr[0:512, 512:1024] = w01[...]
        rhsr[512:1024, 0:512] = jnp.zeros((512, 512), BF)
        rhsr[512:1024, 512:1024] = l1t[...]

    @pl.loop(0, 4)
    def _(n):
        cols = pl.ds(pl.multiple_of(n * 256, 256), 256)

        @pl.when(c != 0)
        def _():
            u1 = (u1p[:, cols] + dot(w01t[...], atb[0:512, cols])).astype(BF)
            rhsr[0:512, cols] = (-(q0p[:, cols] + dot(w01[...], u1))).astype(BF)
            rhsr[512:1024, cols] = (-dot(l1t[...], u1)).astype(BF)

        own = jnp.where(c == 0, 0.0, gcol[:, cols].astype(F32))
        rhsg[:, cols] = ((own + dot(gpan[...], rhsr[:, cols])) * scale).astype(BF)

    out_rhs = [pltpu.make_async_copy(rhsg, rhsg_o, outs.at[1]), pltpu.make_async_copy(rhsr, rhsr_o, outs.at[2])]
    for copy in out_rhs:
        copy.start()

    for t in range(4):

        @pl.when(jnp.logical_or(bits[t] == 1, count == 0))
        def _():
            for q in range(16):
                src = q + (2 if q >= Q01 else 0)
                pltpu.make_async_copy(
                    big.at[t, src], rows_o.at[pl.ds(t * 512 + q * 32, 32)], ld.at[t]
                ).start()

    @pl.loop(0, CT)
    def _(q):
        for t in range(4):

            @pl.when(jnp.logical_and(bits[t] == 0, count > 0))
            def _():
                @pl.when(jnp.logical_or(q < Q01, q >= Q01 + 2))
                def _():
                    hop(t, q, 0).wait_recv()
                    at = 512 * t + 32 * (q - jnp.where(q >= Q01, 2, 0))
                    pltpu.make_async_copy(
                        big.at[t, q], rows_o.at[pl.ds(pl.multiple_of(at, 32), 32)], ld.at[t]
                    ).start()

        for d in range(4):

            @pl.when(sends_on[d])
            def _():
                hop(tree[d], q, d).wait_send()

    out_growt.wait()
    for copy in out_rhs:
        copy.wait()
    for t in range(4):
        whole = rows_o.at[pl.ds(t * 512, 512)]
        pltpu.make_async_copy(whole, whole, ld.at[t]).wait()

    for copy in sends:
        copy.wait_send()

    @pl.when(h != k)
    def _():
        rcopy(my_act, mine, sa_s.at[0], sa_r.at[half, k], partner, c).wait_send()

    @pl.when(k == 0)
    def _():
        for n in range(4):
            for chain in range(2):

                @pl.when(place_of(chain) < 3)
                def _():
                    along(chain, n).wait_send()

                across(chain, n).wait_send()

    for _, _, drain in spreads:
        drain()


def finish(ridge, growt, rows, rhsg, rhsr, out):
    r = lax.axis_index("row")
    c = lax.axis_index("col")
    n = pl.program_id(0)
    height, width = out.shape
    value = dot(growt[...], rhsg[...]) + dot(rows[...], rhsr[...])
    value = value + jnp.where(c == 0, 0.0, ridge[...])
    row_ids = r * 2048 + n * height + lax.broadcasted_iota(jnp.int32, (height, width), 0)
    col_ids = c * 1024 + lax.broadcasted_iota(jnp.int32, (height, width), 1)
    above = jnp.logical_or(
        jnp.logical_and(row_ids < 512, col_ids >= 512), jnp.logical_and(row_ids < 1024, col_ids >= 1024)
    )
    out[...] = jnp.where(above, 0.0, value)


def shape(dims, kind):
    return jax.ShapeDtypeStruct(dims, kind)


VM = pl.BlockSpec(memory_space=pltpu.VMEM)
ANY = pl.BlockSpec(memory_space=pl.ANY)
DMA = pltpu.SemaphoreType.DMA


def per_device(activations, errors, act_proj, err_proj, lengths, ridge, pivot_inverse):
    vmem = pltpu.VMEM
    half = (512, 512)
    growt, rows, rhsg, rhsr = pl.pallas_call(
        exchange,
        out_shape=(
            shape((2048, 512), BF), shape((2048, 1024), BF), shape((512, 1024), BF), shape((1024, 1024), BF)
        ),
        in_specs=[ANY, ANY, VM, VM, VM, ANY, ANY],
        out_specs=(ANY,) * 4,
        scratch_shapes=[
            vmem((1024, 512), BF), vmem((1024, 512), BF), vmem((2, 512, 512), F32), vmem((2048, 1024), F32),
            vmem((4, 16, 32, 128), F32), vmem((4, 8, 32, 128), F32), vmem((4, 4, 32, 128), F32),
            vmem((4, 2, 32, 128), F32), vmem((4, 1, 32, 128), F32),
            vmem((4, 16, 128), BF), vmem((8, 1024), BF), vmem((2, 2, 4, 16, 128), BF),
            vmem((2, 4, 16, 4, 16, 128), BF), vmem((2, 8, 8, 1024), BF), vmem((8, 8, 1024), BF),
            vmem((8, 8, 1024), BF), vmem((1, 1, 1024), jnp.int32), vmem((8, 1, 1024), jnp.int32),
            vmem((4, CT, 32, 1024), BF), vmem((1024, 1024), BF),
        ]
        + [vmem(half, BF)] * 5
        + [
            vmem((512, 2048), BF), vmem((512, 1024), BF), vmem((512, 1024), BF),
            vmem((1024, 512), BF), vmem((2048, 512), BF),
            vmem((1024, 1024), BF), vmem(half, BF), vmem((512, 1024), F32), vmem((512, 1024), F32),
        ]
        + [vmem(half, BF)] * 3
        + [vmem((512, 1024), BF), vmem((1024, 1024), BF)]
        + [
            DMA((4, 4)), DMA((4, 4)), DMA((4, 4)), DMA((4, 4)),
            DMA((4,)), DMA((2, 2)), DMA((8,)), DMA((8,)), DMA((8,)), DMA((8,)),
            DMA((2, 4)), DMA((2, 4)), DMA((2, 4)), DMA((2, 4)),
            DMA((3, 4)), DMA((3, 4)), DMA, DMA,
            DMA((4, CT)), DMA((4, CT)), DMA((8,)), DMA((6,)), DMA((4,)),
        ],
        compiler_params=pltpu.CompilerParams(
            collective_id=0, has_side_effects=True, vmem_limit_bytes=VMEM_LIMIT
        ),
        name="exchange",
    )(activations, errors, act_proj, err_proj, lengths, pivot_inverse, ridge)

    step = 512
    return pl.pallas_call(
        finish,
        out_shape=shape((2048, 1024), F32),
        grid=(2048 // step,),
        in_specs=[
            pl.BlockSpec((step, 1024), lambda n: (n, 0)),
            pl.BlockSpec((step, 512), lambda n: (n, 0)),
            pl.BlockSpec((step, 1024), lambda n: (n, 0)),
            pl.BlockSpec((512, 1024), lambda n: (0, 0)),
            pl.BlockSpec((1024, 1024), lambda n: (0, 0)),
        ],
        out_specs=pl.BlockSpec((step, 1024), lambda n: (n, 0)),
        compiler_params=pltpu.CompilerParams(vmem_limit_bytes=VMEM_LIMIT),
        name="finish",
    )(ridge, growt, rows, rhsg, rhsr)


def solution(mesh):
    in_specs = (
        P("row", "col"), P("row", "col"), P("col", None), P("col", None),
        P("row", None), P("row", "col"), P(),
    )
    return jax.shard_map(
        per_device, mesh=mesh, in_specs=in_specs, out_specs=P("row", "col"), check_vma=False
    )
```

```python
import jax
import jax.numpy as jnp
from jax import lax
from jax.experimental import pallas as pl
from jax.experimental.pallas import tpu as pltpu
from jax.sharding import PartitionSpec as P

MESH = pl.DeviceIdType.MESH
BF = jnp.bfloat16
F32 = jnp.float32
CT = 18
Q01 = 12


def dot(a, b):
    return jnp.dot(a, b, preferred_element_type=F32)


def rcopy(src, dst, ssem, rsem, r, c):
    return pltpu.make_async_remote_copy(
        src_ref=src, dst_ref=dst, send_sem=ssem, recv_sem=rsem, device_id=(r, c), device_id_type=MESH
    )


def flip(v, bit):
    return v + 1 - 2 * (v % 2) if bit == 0 else 3 - v


def gray(v):
    return [((v + 1) // 2) % 2, v // 2]


def order_of(t, c):
    (x0, x1), (y0, y1) = gray(c // 4), gray(c % 4)
    bits = [x0, y0, x1, y1]
    return sum(bits[(t + n) % 4] * (8 >> n) for n in range(4))


def trees_of(bits):
    count = bits[0] + bits[1] + bits[2] + bits[3]
    tree = []
    for d in range(4):
        d1, d2, d3 = (d + 1) % 4, (d + 2) % 4, (d + 3) % 4
        up = jnp.where(bits[d1] == 1, d1, jnp.where(bits[d2] == 1, d2, jnp.where(bits[d3] == 1, d3, d)))
        tree.append(jnp.where(bits[d] == 1, d, up))
    return tree, [jnp.logical_or(bits[d] == 0, count > 1) for d in range(4)]


def exchange(
    acts, errs, actp_in, errp_in, lens_in, piv_in, ridge,
    growt, rows, rhsg, rhsr,
    av, ev, actp, errp, lens, piv, stage, part, in0, in1, in2, in3, my_act, my_err, near, act, erow, ecol, epan, cap, capall, rfirst, colp,
    l0, l0t, l1, l1t, s0, grow, gcol, gpan, gpt, atb, r01, w01, w01t,
    rs_s, rs_r, ag_s, ag_r, sa_s, sa_r, se_s, se_r, cp_s, cp_r,
    cz_s, cz_r, cd_s, cd_r,
    sp_s, sp_r, d2_s, d2_r,
    ts, tr, ld, loc,
):
    r = lax.axis_index("row")
    c = lax.axis_index("col")
    z, k = r // 2, r % 2
    x, y = c // 4, c % 4
    partner = 2 * z + 1 - k

    get_act = pltpu.make_async_copy(acts, av, loc.at[0])
    get_err = pltpu.make_async_copy(errs, ev, loc.at[1])
    get_piv = pltpu.make_async_copy(piv_in, piv, loc.at[2])
    small = [
        pltpu.make_async_copy(src, dst, loc.at[3 + n])
        for n, (src, dst) in enumerate(((actp_in, actp), (errp_in, errp), (lens_in, lens)))
    ]
    small[0].start()
    get_act.start()
    small[1].start()
    get_err.start()
    small[2].start()

    def row_of(dz, dk):
        return 2 * ((z + dz) % 4) + (k + dk) % 2

    def xcol(d):
        return 4 * ((x + d) % 4) + y

    def ycol(d):
        return 4 * x + (y + d) % 4

    column = [(dz, dk) for dz in range(4) for dk in range(2) if dz or dk]
    loads = [
        pltpu.make_async_copy(ridge.at[pl.ds(n * 256, 256)], stage.at[pl.ds(n * 256, 256)], ld.at[n])
        for n in range(8)
    ]

    bits = [gray(x)[0], gray(y)[0], gray(x)[1], gray(y)[1]]
    count = bits[0] + bits[1] + bits[2] + bits[3]
    nbr = [4 * flip(x, 0) + y, 4 * x + flip(y, 0), 4 * flip(x, 1) + y, 4 * x + flip(y, 1)]

    barrier = pltpu.get_barrier_semaphore()
    for d in range(1, 16):
        pl.semaphore_signal(barrier, inc=1, device_id=(r, (c + d) % 16), device_id_type=MESH)
    for dz, dk in column:
        pl.semaphore_signal(barrier, inc=1, device_id=(row_of(dz, dk), c), device_id_type=MESH)

    small[0].wait()
    get_act.wait()
    part[:, :, 0:16, :] = dot(av[...], actp[...]).reshape(4, 16, 16, 128)
    small[1].wait()
    small[2].wait()
    get_err.wait()
    get_piv.start()

    @pl.when(jnp.logical_or(c == 0, r == 0))
    def _():
        for copy in loads:
            copy.start()

    turned_proj = errp[...].T
    for t in range(4):
        out = lax.dot_general(
            turned_proj, ev[t * 256 : (t + 1) * 256, :], (((1,), (1,)), ((), ())), preferred_element_type=F32
        )
        for n in range(16):
            part[t, order_of(t, n), 16:24, :] = out[8 * n : 8 * n + 8, 0:128]
            part[t, order_of(t, n), 24:32, :] = out[8 * n : 8 * n + 8, 128:256]

    lower = lax.broadcasted_iota(jnp.int32, (64, 64), 1) <= lax.broadcasted_iota(jnp.int32, (64, 64), 0)
    ends = jnp.sum(jnp.where(lower, lens[...].astype(F32), 0.0), axis=1, keepdims=True)
    past = lax.broadcasted_iota(jnp.int32, (64, 1024), 1).astype(F32) >= ends
    cap[0] = jnp.sum(past.astype(F32), axis=0, keepdims=True).astype(jnp.int32)

    pl.semaphore_wait(barrier, 22)

    sends = []

    def go(copy):
        copy.start()
        sends.append(copy)

    landing = [in0, in1, in2, in3]
    base = [[jnp.int32(0)] * 4]
    for n in range(4):
        base.append([base[n][t] + bits[(t + n) % 4] * (8 >> n) for t in range(4)])

    def halve(n, t):
        d, size = (t + n) % 4, 8 >> n
        away = base[n][t] + (1 - bits[d]) * size
        return rcopy(
            part.at[t, pl.ds(away, size)], landing[n].at[t], rs_s.at[n, t], rs_r.at[n, t], r, nbr[d]
        )

    def send_halves(n):
        for t in range(4):
            go(halve(n, t))

    def add_halves(n):
        size = 8 >> n
        for t in range(4):
            halve(n, t).wait_recv()
            keep = pl.ds(base[n + 1][t], size)
            part[t, keep] = part[t, keep] + landing[n][t]

    send_halves(0)
    for dz, dk in column:
        n = 2 * dz + dk
        go(rcopy(cap.at[0], capall.at[r], cp_s.at[n], cp_r.at[n], row_of(dz, dk), c))
    own_cap = pltpu.make_async_copy(cap.at[0], capall.at[r], loc.at[0])
    own_cap.start()

    @pl.when(jnp.logical_or(c == 0, r == 0))
    def _():
        for copy in loads:
            copy.wait()

    @pl.when(r == 0)
    def _():
        @pl.loop(0, 16)
        def _(n):
            some = pl.ds(pl.multiple_of(n * 64, 64), 64)
            colp[some, :] = stage[some, :].astype(BF)

    @pl.when(c == 0)
    def _():
        @pl.loop(0, 32)
        def _(n):
            some = pl.ds(pl.multiple_of(n * 64, 64), 64)
            rows[some, :] = stage[some, :].astype(BF)

    def piece(chain, n):
        return colp.at[pl.ds(pl.multiple_of(chain * 512 + n * 128, 128), 128)]

    def place_of(chain):
        return z if chain == 0 else (4 - z) % 4

    def along(chain, n):
        follow = 2 * ((z + 1) % 4) if chain == 0 else 2 * ((z + 3) % 4)
        return rcopy(piece(chain, n), piece(chain, n), cz_s.at[chain, n], cz_r.at[chain, n], follow, c)

    def across(chain, n):
        return rcopy(piece(chain, n), piece(chain, n), cd_s.at[chain, n], cd_r.at[chain, n], partner, c)

    @pl.when(r == 0)
    def _():
        for n in range(4):
            for chain in range(2):
                along(chain, n).start()
                across(chain, n).start()

    def chain_round(j):
        for chain in range(2):
            place = place_of(chain)
            n = j - jnp.where(place == 2, 2, 0)
            inner = jnp.logical_or(place == 1, place == 2)
            on = jnp.logical_and(inner, jnp.logical_and(n >= 0, n < 4))

            @pl.when(jnp.logical_and(k == 0, on))
            def _():
                along(chain, n).wait_recv()
                along(chain, n).start()
                across(chain, n).start()

    def chain_ends():
        for n in range(4):
            for chain in range(2):

                @pl.when(jnp.logical_and(k == 0, place_of(chain) == 3))
                def _():
                    along(chain, n).wait_recv()
                    across(chain, n).start()

                @pl.when(k == 1)
                def _():
                    across(chain, n).wait_recv()

    tree, sends_on = trees_of(bits)

    def is_first(q):
        return jnp.logical_and(q >= Q01, q < Q01 + 2)

    def hop(t, q, d, first):
        if first:
            chunk = rfirst.at[t, q - Q01]
        else:
            at = t * 512 + 32 * (q - jnp.where(q >= Q01, 2, 0))
            chunk = rows.at[pl.ds(pl.multiple_of(at, 32), 32)]
        return rcopy(chunk, chunk, ts.at[d, q], tr.at[t, q], r, nbr[d])

    def step(s):
        q = s - 2 * count
        for first in (False, True):

            @pl.when(jnp.logical_and(jnp.logical_and(q >= 0, q < CT), is_first(q) == first))
            def _():
                for t in range(4):

                    @pl.when(bits[t] == 1)
                    def _():
                        hop(t, q, 0, first).wait_recv()

                for d in range(4):

                    @pl.when(sends_on[d])
                    def _():
                        hop(tree[d], q, d, first).start()

    step(0)
    step(1)
    get_piv.wait()
    for src, plain, turned in ((piv.at[0], l0, l0t), (piv.at[1], l1, l1t)):
        plain[...] = src[...].astype(BF)
        turned[...] = src[...].T.astype(BF)
    s0[...] = dot(l0t[...], l0[...]).astype(BF)

    add_halves(0)
    send_halves(1)
    chain_round(0)
    step(2)
    add_halves(1)
    send_halves(2)
    chain_round(1)
    step(3)
    add_halves(2)
    send_halves(3)
    chain_round(2)
    step(4)
    add_halves(3)
    for t in range(4):
        block = part[t, base[4][t]].astype(BF)
        my_act[t] = block[0:16]
        my_err[:, t * 256 : t * 256 + 128] = part[t, base[4][t], 16:24, :].astype(BF)
        my_err[:, t * 256 + 128 : t * 256 + 256] = part[t, base[4][t], 24:32, :].astype(BF)

    h, half = z // 2, z % 2
    mine = near.at[half, k]
    own_act = pltpu.make_async_copy(my_act, mine, loc.at[1])
    own_err = pltpu.make_async_copy(my_err, ecol.at[r], loc.at[2])
    own_err.start()

    @pl.when(h == k)
    def _():
        own_act.start()

    @pl.when(h != k)
    def _():
        rcopy(my_act, mine, sa_s.at[0], sa_r.at[half, k], partner, c).start()

    for dz in range(1, 4):
        go(rcopy(my_act, mine, sa_s.at[dz], sa_r.at[half, k], 2 * ((z + dz) % 4) + h, c))
    for dz, dk in column:
        n = 2 * dz + dk
        go(rcopy(my_err, ecol.at[r], se_s.at[n], se_r.at[n], row_of(dz, dk), c))

    chain_round(3)
    step(5)
    step(6)

    for i in range(2):
        for j in range(2):
            away = jnp.logical_or(z != 2 * k + i, k != j)

            @pl.when(away)
            def _():
                rcopy(my_act, near.at[i, j], sa_s.at[0], sa_r.at[i, j], partner, c).wait_recv()

    @pl.when(h == k)
    def _():
        own_act.wait()

    for t in range(4):
        for i in range(2):
            for j in range(2):
                act[k, t, base[4][t], 2 * i + j] = near[i, j, t]

    def double(n, t):
        d, size = (t + n) % 4, 8 >> n
        held = act.at[k, t, pl.ds(base[n + 1][t], size)]
        return rcopy(held, held, ag_s.at[n, t], ag_r.at[n, t], r, nbr[d])

    def send_doubles(n):
        for t in range(4):
            go(double(n, t))

    def wait_doubles(n):
        size = 8 >> n
        for t in range(4):
            other = base[n][t] + (1 - bits[(t + n) % 4]) * size
            held = act.at[k, t, pl.ds(other, size)]
            rcopy(held, held, ag_s.at[n, t], ag_r.at[n, t], r, nbr[0]).wait_recv()

    send_doubles(3)
    own_err.wait()
    for dz, dk in column:
        n = 2 * dz + dk
        rcopy(my_err, ecol.at[row_of(4 - dz, 2 - dk)], se_s.at[n], se_r.at[n], partner, c).wait_recv()

    def spread(m, buf, from_x, from_y):
        root = [gray(from_x)[0], gray(from_y)[0], gray(from_x)[1], gray(from_y)[1]]
        rel = [bits[d] + root[d] - 2 * bits[d] * root[d] for d in range(4)]
        far = rel[0] + rel[1] + rel[2] + rel[3]
        which, on = trees_of(rel)

        def send(t, d):
            quarter = buf.at[pl.ds(2 * t, 2)]
            return rcopy(quarter, quarter, sp_s.at[m, d], sp_r.at[m, t], r, nbr[d])

        def relay(depth):
            @pl.when(far == depth)
            def _():
                if depth == 0:
                    copy = pltpu.make_async_copy(ecol, buf, loc.at[3])
                    copy.start()
                    copy.wait()
                for t in range(4):
                    if depth:

                        @pl.when(rel[t] == 1)
                        def _():
                            send(t, 0).wait_recv()

                for d in range(4):

                    @pl.when(on[d])
                    def _():
                        send(which[d], d).start()

        def finish():
            for t in range(4):

                @pl.when(jnp.logical_and(rel[t] == 0, far > 0))
                def _():
                    send(t, 0).wait_recv()

        def drain():
            for d in range(4):

                @pl.when(on[d])
                def _():
                    send(which[d], d).wait_send()

        return relay, finish, drain

    spreads = [
        spread(0, erow.at[0], z, 2 * k), spread(1, erow.at[1], z, 2 * k + 1),
        spread(2, epan, jnp.int32(0), jnp.int32(0)),
    ]

    def relay_all(depth):
        for relay, _, _ in spreads:
            relay(depth)

    relay_all(0)
    chain_round(4)
    step(7)
    wait_doubles(3)
    send_doubles(2)
    relay_all(1)
    chain_round(5)
    step(8)

    wait_doubles(2)
    send_doubles(1)
    relay_all(2)
    step(9)
    wait_doubles(1)
    send_doubles(0)
    relay_all(3)
    step(10)
    chain_ends()

    @pl.when(c == 0)
    def _():
        for t in range(4):
            for u in range(2):
                for b in range(2):
                    at = 256 * b + 64 * t + 32 * u
                    rfirst[t, u, :, b * 512 : (b + 1) * 512] = colp[at : at + 32, 512:1024]

    step(11)
    wait_doubles(0)
    go(rcopy(act.at[k], act.at[k], d2_s, d2_r, partner, c))

    relay_all(4)
    for _, finish_spread, _ in spreads:
        finish_spread()

    own_cap.wait()
    for dz, dk in column:
        n = 2 * dz + dk
        rcopy(cap.at[0], capall.at[row_of(4 - dz, 2 - dk)], cp_s.at[n], cp_r.at[n], partner, c).wait_recv()

    def gradients(h, n):
        q = h * 4 + n
        right = jnp.concatenate([act[h, t, :, n].reshape(256, 128) for t in range(4)], axis=0)
        ids = lax.broadcasted_iota(jnp.int32, (64, 1024), 0)
        member = (capall[q] == ids).astype(F32).astype(BF)
        spot = pl.ds(pl.multiple_of(q * 64, 64), 64)
        for src, dst, base in (
            (erow.at[0], grow, 0), (erow.at[1], grow, 1024), (ecol, gcol, 0), (epan, gpan, 0),
        ):
            e8 = src[q]
            left = jnp.concatenate([member * e8[i : i + 1, :] for i in range(8)], axis=0)
            out = dot(left, right).astype(BF)
            for i in range(8):
                dst[spot, base + i * 128 : base + (i + 1) * 128] = out[i * 64 : (i + 1) * 64]

    @pl.loop(0, 2)
    def _(i):
        @pl.when(i == 1)
        def _():
            rcopy(act.at[k], act.at[1 - k], d2_s, d2_r, partner, c).wait_recv()

        for n in range(4):
            gradients((k + i) % 2, n)
            step(12 + 4 * i + n)

    scale = 1.0 / 512.0
    for n in range(2):
        gpt[n * 512 : (n + 1) * 512, :] = gpan[:, n * 512 : (n + 1) * 512].T
    step(20)
    step(21)
    for n in range(4):
        growt[n * 512 : (n + 1) * 512, :] = grow[:, n * 512 : (n + 1) * 512].T

    u1p, q0p = stage.at[pl.ds(0, 512)], stage.at[pl.ds(512, 512)]
    for n in range(2):

        @pl.when(c != 0)
        def _():
            for cols in (slice(n * 512, n * 512 + 256), slice(n * 512 + 256, n * 512 + 512)):
                at = (colp[:, cols].astype(F32) + dot(gpt[...], gcol[:, cols]) * scale).astype(BF)
                atb[:, cols] = at
                u0 = dot(l0[...], at[0:512]).astype(BF)
                u1p[:, cols] = dot(l1[...], at[512:1024])
                q0p[:, cols] = dot(l0t[...], u0)

        step(22 + 2 * n)
        step(23 + 2 * n)

    for u in range(2):
        for t in range(4):

            @pl.when(jnp.logical_and(bits[t] == 0, count > 0))
            def _():
                hop(t, Q01 + u, 0, True).wait_recv()

    for t in range(4):
        for u in range(2):
            for b in range(2):
                at = 256 * b + 64 * t + 32 * u
                r01[at : at + 32, :] = rfirst[t, u, :, b * 512 : (b + 1) * 512]
    a01 = (r01[...].astype(F32) + dot(gpt[0:512, :], gpan[:, 512:1024]) * scale).astype(BF)
    corner = -dot(dot(s0[...], a01).astype(BF), l1t[...])
    w01[...] = corner.astype(BF)
    w01t[...] = corner.T.astype(BF)

    @pl.when(c == 0)
    def _():
        rhsr[0:512, 0:512] = l0t[...]
        rhsr[0:512, 512:1024] = w01[...]
        rhsr[512:1024, 0:512] = jnp.zeros((512, 512), BF)
        rhsr[512:1024, 512:1024] = l1t[...]

    @pl.when(c != 0)
    def _():
        for n in range(4):
            cols = slice(n * 256, n * 256 + 256)
            u1 = (u1p[:, cols] + dot(w01t[...], atb[0:512, cols])).astype(BF)
            rhsr[0:512, cols] = (-(q0p[:, cols] + dot(w01[...], u1))).astype(BF)
            rhsr[512:1024, cols] = (-dot(l1t[...], u1)).astype(BF)

    for n in range(4):
        cols = slice(n * 256, n * 256 + 256)
        own = jnp.where(c == 0, 0.0, gcol[:, cols].astype(F32))
        rhsg[:, cols] = ((own + dot(gpan[...], rhsr[:, cols])) * scale).astype(BF)

    @pl.loop(0, CT)
    def _(q):
        for t in range(4):

            @pl.when(jnp.logical_and(jnp.logical_and(bits[t] == 0, count > 0), jnp.logical_not(is_first(q))))
            def _():
                hop(t, q, 0, False).wait_recv()

        for d in range(4):
            for first in (False, True):

                @pl.when(jnp.logical_and(sends_on[d], is_first(q) == first))
                def _():
                    hop(tree[d], q, d, first).wait_send()

    for copy in sends:
        copy.wait_send()

    @pl.when(h != k)
    def _():
        rcopy(my_act, mine, sa_s.at[0], sa_r.at[half, k], partner, c).wait_send()

    @pl.when(k == 0)
    def _():
        for n in range(4):
            for chain in range(2):

                @pl.when(place_of(chain) < 3)
                def _():
                    along(chain, n).wait_send()

                across(chain, n).wait_send()

    for _, _, drain in spreads:
        drain()


def finish(ridge, growt, rows, rhsg, rhsr, out):
    r = lax.axis_index("row")
    c = lax.axis_index("col")
    n = pl.program_id(0)
    height, width = out.shape
    some = pl.ds(pl.multiple_of(n * height, height), height)
    value = dot(growt[some, :], rhsg[...]) + dot(rows[some, :], rhsr[...])
    value = value + jnp.where(c == 0, 0.0, ridge[...])
    row_ids = r * 2048 + n * height + lax.broadcasted_iota(jnp.int32, (height, width), 0)
    col_ids = c * 1024 + lax.broadcasted_iota(jnp.int32, (height, width), 1)
    above = jnp.logical_or(
        jnp.logical_and(row_ids < 512, col_ids >= 512), jnp.logical_and(row_ids < 1024, col_ids >= 1024)
    )
    out[...] = jnp.where(above, 0.0, value)


def shape(dims, kind):
    return jax.ShapeDtypeStruct(dims, kind)


VM = pl.BlockSpec(memory_space=pltpu.VMEM)
ANY = pl.BlockSpec(memory_space=pl.ANY)
HBM = pl.BlockSpec(memory_space=pltpu.HBM)
DMA = pltpu.SemaphoreType.DMA


def per_device(activations, errors, act_proj, err_proj, lengths, ridge, pivot_inverse):
    vmem = pltpu.VMEM
    half = (512, 512)
    args = [
        pltpu.with_memory_space_constraint(a, pltpu.HBM)
        for a in (activations, errors, act_proj, err_proj, lengths, pivot_inverse, ridge)
    ]
    growt, rows, rhsg, rhsr = pl.pallas_call(
        exchange,
        out_shape=(
            vmem((2048, 512), BF), vmem((2048, 1024), BF), vmem((512, 1024), BF), vmem((1024, 1024), BF)
        ),
        in_specs=[HBM, HBM, HBM, HBM, HBM, HBM, HBM],
        out_specs=(VM,) * 4,
        scratch_shapes=[
            vmem((1024, 512), BF), vmem((1024, 512), BF), vmem((512, 128), BF), vmem((512, 128), BF),
            vmem((1, 64), jnp.int32), vmem((2, 512, 512), F32), vmem((2048, 1024), F32),
            vmem((4, 16, 32, 128), F32), vmem((4, 8, 32, 128), F32), vmem((4, 4, 32, 128), F32),
            vmem((4, 2, 32, 128), F32), vmem((4, 1, 32, 128), F32),
            vmem((4, 16, 128), BF), vmem((8, 1024), BF), vmem((2, 2, 4, 16, 128), BF),
            vmem((2, 4, 16, 4, 16, 128), BF), vmem((2, 8, 8, 1024), BF), vmem((8, 8, 1024), BF),
            vmem((8, 8, 1024), BF), vmem((1, 1, 1024), jnp.int32), vmem((8, 1, 1024), jnp.int32),
            vmem((4, 2, 32, 1024), BF), vmem((1024, 1024), BF),
        ]
        + [vmem(half, BF)] * 5
        + [
            vmem((512, 2048), BF), vmem((512, 1024), BF), vmem((512, 1024), BF),
            vmem((1024, 512), BF),
            vmem((1024, 1024), BF),
        ]
        + [vmem(half, BF)] * 3
        + [
            DMA((4, 4)), DMA((4, 4)), DMA((4, 4)), DMA((4, 4)),
            DMA((4,)), DMA((2, 2)), DMA((8,)), DMA((8,)), DMA((8,)), DMA((8,)),
            DMA((2, 4)), DMA((2, 4)), DMA((2, 4)), DMA((2, 4)),
            DMA((3, 4)), DMA((3, 4)), DMA, DMA,
            DMA((4, CT)), DMA((4, CT)), DMA((8,)), DMA((6,)),
        ],
        compiler_params=pltpu.CompilerParams(
            collective_id=0, has_side_effects=True, vmem_limit_bytes=44 << 20
        ),
        name="exchange",
    )(*args)

    step = 512
    return pl.pallas_call(
        finish,
        out_shape=shape((2048, 1024), F32),
        grid=(2048 // step,),
        in_specs=[
            pl.BlockSpec((step, 1024), lambda n: (n, 0)),
            VM, VM, VM, VM,
        ],
        out_specs=pl.BlockSpec((step, 1024), lambda n: (n, 0)),
        compiler_params=pltpu.CompilerParams(vmem_limit_bytes=20 << 20),
        name="finish",
    )(ridge, *(pltpu.with_memory_space_constraint(a, pltpu.VMEM) for a in (growt, rows, rhsg, rhsr)))


def solution(mesh):
    in_specs = (
        P("row", "col"), P("row", "col"), P("col", None), P("col", None),
        P("row", None), P("row", "col"), P(),
    )
    return jax.shard_map(
        per_device, mesh=mesh, in_specs=in_specs, out_specs=P("row", "col"), check_vma=False
    )
```

```python
import jax
import jax.numpy as jnp
from jax import lax
from jax.experimental import pallas as pl
from jax.experimental.pallas import tpu as pltpu
from jax.sharding import PartitionSpec as P

MESH = pl.DeviceIdType.MESH
BF = jnp.bfloat16
F32 = jnp.float32
CT = 18
Q01 = 12


def dot(a, b):
    return jnp.dot(a, b, preferred_element_type=F32)


def rcopy(src, dst, ssem, rsem, r, c):
    return pltpu.make_async_remote_copy(
        src_ref=src, dst_ref=dst, send_sem=ssem, recv_sem=rsem, device_id=(r, c), device_id_type=MESH
    )


def flip(v, bit):
    return v + 1 - 2 * (v % 2) if bit == 0 else 3 - v


def gray(v):
    return [((v + 1) // 2) % 2, v // 2]


def order_of(t, c):
    (x0, x1), (y0, y1) = gray(c // 4), gray(c % 4)
    bits = [x0, y0, x1, y1]
    return sum(bits[(t + n) % 4] * (8 >> n) for n in range(4))


def trees_of(bits):
    count = bits[0] + bits[1] + bits[2] + bits[3]
    tree = []
    for d in range(4):
        d1, d2, d3 = (d + 1) % 4, (d + 2) % 4, (d + 3) % 4
        up = jnp.where(bits[d1] == 1, d1, jnp.where(bits[d2] == 1, d2, jnp.where(bits[d3] == 1, d3, d)))
        tree.append(jnp.where(bits[d] == 1, d, up))
    return tree, [jnp.logical_or(bits[d] == 0, count > 1) for d in range(4)]


def exchange(
    acts, errs, actp_in, errp_in, lens_in, piv_in, ridge,
    growt, rows, rhsg, rhsr,
    av, ev, actp, errp, lens, piv, stage, part, in0, in1, in2, in3, my_act, my_err, near, act, erow, ecol, epan, cap, capall, rfirst, colp,
    l0, l0t, l1, l1t, s0, grow, gcol, gpan, gpt, atb, r01, w01, w01t,
    rs_s, rs_r, ag_s, ag_r, sa_s, sa_r, se_s, se_r, cp_s, cp_r,
    cz_s, cz_r, cd_s, cd_r,
    sp_s, sp_r, d2_s, d2_r,
    ts, tr, ld, loc,
):
    r = lax.axis_index("row")
    c = lax.axis_index("col")
    z, k = r // 2, r % 2
    x, y = c // 4, c % 4
    partner = 2 * z + 1 - k

    get_act = pltpu.make_async_copy(acts, av, loc.at[0])
    get_err = pltpu.make_async_copy(errs, ev, loc.at[1])
    get_piv = pltpu.make_async_copy(piv_in, piv, loc.at[2])
    small = [
        pltpu.make_async_copy(src, dst, loc.at[3 + n])
        for n, (src, dst) in enumerate(((actp_in, actp), (errp_in, errp), (lens_in, lens)))
    ]
    small[0].start()
    get_act.start()
    small[1].start()
    get_err.start()
    small[2].start()

    def row_of(dz, dk):
        return 2 * ((z + dz) % 4) + (k + dk) % 2

    def xcol(d):
        return 4 * ((x + d) % 4) + y

    def ycol(d):
        return 4 * x + (y + d) % 4

    column = [(dz, dk) for dz in range(4) for dk in range(2) if dz or dk]
    loads = [
        pltpu.make_async_copy(ridge.at[pl.ds(n * 256, 256)], stage.at[pl.ds(n * 256, 256)], ld.at[n])
        for n in range(8)
    ]

    bits = [gray(x)[0], gray(y)[0], gray(x)[1], gray(y)[1]]
    count = bits[0] + bits[1] + bits[2] + bits[3]
    nbr = [4 * flip(x, 0) + y, 4 * x + flip(y, 0), 4 * flip(x, 1) + y, 4 * x + flip(y, 1)]

    barrier = pltpu.get_barrier_semaphore()
    for d in range(1, 16):
        pl.semaphore_signal(barrier, inc=1, device_id=(r, (c + d) % 16), device_id_type=MESH)
    for dz, dk in column:
        pl.semaphore_signal(barrier, inc=1, device_id=(row_of(dz, dk), c), device_id_type=MESH)

    small[0].wait()
    get_act.wait()
    part[:, :, 0:16, :] = dot(av[...], actp[...]).reshape(4, 16, 16, 128)
    small[1].wait()
    small[2].wait()
    get_err.wait()
    get_piv.start()

    @pl.when(jnp.logical_or(c == 0, r == 0))
    def _():
        for copy in loads:
            copy.start()

    turned_proj = errp[...].T
    for t in range(4):
        out = lax.dot_general(
            turned_proj, ev[t * 256 : (t + 1) * 256, :], (((1,), (1,)), ((), ())), preferred_element_type=F32
        )
        for n in range(16):
            part[t, order_of(t, n), 16:24, :] = out[8 * n : 8 * n + 8, 0:128]
            part[t, order_of(t, n), 24:32, :] = out[8 * n : 8 * n + 8, 128:256]

    lower = lax.broadcasted_iota(jnp.int32, (64, 64), 1) <= lax.broadcasted_iota(jnp.int32, (64, 64), 0)
    ends = jnp.sum(jnp.where(lower, lens[...].astype(F32), 0.0), axis=1, keepdims=True)
    past = lax.broadcasted_iota(jnp.int32, (64, 1024), 1).astype(F32) >= ends
    cap[0] = jnp.sum(past.astype(F32), axis=0, keepdims=True).astype(jnp.int32)

    pl.semaphore_wait(barrier, 22)

    sends = []

    def go(copy):
        copy.start()
        sends.append(copy)

    landing = [in0, in1, in2, in3]
    base = [[jnp.int32(0)] * 4]
    for n in range(4):
        base.append([base[n][t] + bits[(t + n) % 4] * (8 >> n) for t in range(4)])

    def halve(n, t):
        d, size = (t + n) % 4, 8 >> n
        away = base[n][t] + (1 - bits[d]) * size
        return rcopy(
            part.at[t, pl.ds(away, size)], landing[n].at[t], rs_s.at[n, t], rs_r.at[n, t], r, nbr[d]
        )

    def send_halves(n):
        for t in range(4):
            go(halve(n, t))

    def add_halves(n):
        size = 8 >> n
        for t in range(4):
            halve(n, t).wait_recv()
            keep = pl.ds(base[n + 1][t], size)
            part[t, keep] = part[t, keep] + landing[n][t]

    send_halves(0)
    for dz, dk in column:
        n = 2 * dz + dk
        go(rcopy(cap.at[0], capall.at[r], cp_s.at[n], cp_r.at[n], row_of(dz, dk), c))
    own_cap = pltpu.make_async_copy(cap.at[0], capall.at[r], loc.at[0])
    own_cap.start()

    @pl.when(jnp.logical_or(c == 0, r == 0))
    def _():
        for copy in loads:
            copy.wait()

    @pl.when(r == 0)
    def _():
        @pl.loop(0, 16)
        def _(n):
            some = pl.ds(pl.multiple_of(n * 64, 64), 64)
            colp[some, :] = stage[some, :].astype(BF)

    @pl.when(c == 0)
    def _():
        @pl.loop(0, 32)
        def _(n):
            some = pl.ds(pl.multiple_of(n * 64, 64), 64)
            rows[some, :] = stage[some, :].astype(BF)

    def piece(chain, n):
        return colp.at[pl.ds(pl.multiple_of(chain * 512 + n * 128, 128), 128)]

    def place_of(chain):
        return z if chain == 0 else (4 - z) % 4

    def along(chain, n):
        follow = 2 * ((z + 1) % 4) if chain == 0 else 2 * ((z + 3) % 4)
        return rcopy(piece(chain, n), piece(chain, n), cz_s.at[chain, n], cz_r.at[chain, n], follow, c)

    def across(chain, n):
        return rcopy(piece(chain, n), piece(chain, n), cd_s.at[chain, n], cd_r.at[chain, n], partner, c)

    @pl.when(r == 0)
    def _():
        for n in range(4):
            for chain in range(2):
                along(chain, n).start()
                across(chain, n).start()

    def chain_round(j):
        for chain in range(2):
            place = place_of(chain)
            n = j - jnp.where(place == 2, 2, 0)
            inner = jnp.logical_or(place == 1, place == 2)
            on = jnp.logical_and(inner, jnp.logical_and(n >= 0, n < 4))

            @pl.when(jnp.logical_and(k == 0, on))
            def _():
                along(chain, n).wait_recv()
                along(chain, n).start()
                across(chain, n).start()

    def chain_ends():
        for n in range(4):
            for chain in range(2):

                @pl.when(jnp.logical_and(k == 0, place_of(chain) == 3))
                def _():
                    along(chain, n).wait_recv()
                    across(chain, n).start()

                @pl.when(k == 1)
                def _():
                    across(chain, n).wait_recv()

    tree, sends_on = trees_of(bits)

    def is_first(q):
        return jnp.logical_and(q >= Q01, q < Q01 + 2)

    def hop(t, q, d, first):
        if first:
            chunk = rfirst.at[t, q - Q01]
        else:
            at = t * 512 + 32 * (q - jnp.where(q >= Q01, 2, 0))
            chunk = rows.at[pl.ds(pl.multiple_of(at, 32), 32)]
        return rcopy(chunk, chunk, ts.at[d, q], tr.at[t, q], r, nbr[d])

    def step(s):
        q = s - 2 * count
        for first in (False, True):

            @pl.when(jnp.logical_and(jnp.logical_and(q >= 0, q < CT), is_first(q) == first))
            def _():
                for t in range(4):

                    @pl.when(bits[t] == 1)
                    def _():
                        hop(t, q, 0, first).wait_recv()

                for d in range(4):

                    @pl.when(sends_on[d])
                    def _():
                        hop(tree[d], q, d, first).start()

    step(0)
    step(1)
    get_piv.wait()
    for src, plain, turned in ((piv.at[0], l0, l0t), (piv.at[1], l1, l1t)):
        plain[...] = src[...].astype(BF)
        turned[...] = src[...].T.astype(BF)
    s0[...] = dot(l0t[...], l0[...]).astype(BF)

    add_halves(0)
    send_halves(1)
    chain_round(0)
    step(2)
    add_halves(1)
    send_halves(2)
    chain_round(1)
    step(3)
    add_halves(2)
    send_halves(3)
    chain_round(2)
    step(4)
    add_halves(3)
    for t in range(4):
        block = part[t, base[4][t]].astype(BF)
        my_act[t] = block[0:16]
        my_err[:, t * 256 : t * 256 + 128] = part[t, base[4][t], 16:24, :].astype(BF)
        my_err[:, t * 256 + 128 : t * 256 + 256] = part[t, base[4][t], 24:32, :].astype(BF)

    h, half = z // 2, z % 2
    mine = near.at[half, k]
    own_act = pltpu.make_async_copy(my_act, mine, loc.at[1])
    own_err = pltpu.make_async_copy(my_err, ecol.at[r], loc.at[2])
    own_err.start()

    @pl.when(h == k)
    def _():
        own_act.start()

    @pl.when(h != k)
    def _():
        rcopy(my_act, mine, sa_s.at[0], sa_r.at[half, k], partner, c).start()

    for dz in range(1, 4):
        go(rcopy(my_act, mine, sa_s.at[dz], sa_r.at[half, k], 2 * ((z + dz) % 4) + h, c))
    for dz, dk in column:
        n = 2 * dz + dk
        go(rcopy(my_err, ecol.at[r], se_s.at[n], se_r.at[n], row_of(dz, dk), c))

    chain_round(3)
    step(5)
    step(6)

    for i in range(2):
        for j in range(2):
            away = jnp.logical_or(z != 2 * k + i, k != j)

            @pl.when(away)
            def _():
                rcopy(my_act, near.at[i, j], sa_s.at[0], sa_r.at[i, j], partner, c).wait_recv()

    @pl.when(h == k)
    def _():
        own_act.wait()

    for t in range(4):
        for i in range(2):
            for j in range(2):
                act[k, t, base[4][t], 2 * i + j] = near[i, j, t]

    def double(n, t):
        d, size = (t + n) % 4, 8 >> n
        held = act.at[k, t, pl.ds(base[n + 1][t], size)]
        return rcopy(held, held, ag_s.at[n, t], ag_r.at[n, t], r, nbr[d])

    def send_doubles(n):
        for t in range(4):
            go(double(n, t))

    def wait_doubles(n):
        size = 8 >> n
        for t in range(4):
            other = base[n][t] + (1 - bits[(t + n) % 4]) * size
            held = act.at[k, t, pl.ds(other, size)]
            rcopy(held, held, ag_s.at[n, t], ag_r.at[n, t], r, nbr[0]).wait_recv()

    send_doubles(3)
    own_err.wait()
    for dz, dk in column:
        n = 2 * dz + dk
        rcopy(my_err, ecol.at[row_of(4 - dz, 2 - dk)], se_s.at[n], se_r.at[n], partner, c).wait_recv()

    def spread(m, buf, from_x, from_y):
        root = [gray(from_x)[0], gray(from_y)[0], gray(from_x)[1], gray(from_y)[1]]
        rel = [bits[d] + root[d] - 2 * bits[d] * root[d] for d in range(4)]
        far = rel[0] + rel[1] + rel[2] + rel[3]
        which, on = trees_of(rel)

        def send(t, d):
            quarter = buf.at[pl.ds(2 * t, 2)]
            return rcopy(quarter, quarter, sp_s.at[m, d], sp_r.at[m, t], r, nbr[d])

        def relay(depth):
            @pl.when(far == depth)
            def _():
                if depth == 0:
                    copy = pltpu.make_async_copy(ecol, buf, loc.at[3])
                    copy.start()
                    copy.wait()
                for t in range(4):
                    if depth:

                        @pl.when(rel[t] == 1)
                        def _():
                            send(t, 0).wait_recv()

                for d in range(4):

                    @pl.when(on[d])
                    def _():
                        send(which[d], d).start()

        def finish():
            for t in range(4):

                @pl.when(jnp.logical_and(rel[t] == 0, far > 0))
                def _():
                    send(t, 0).wait_recv()

        def drain():
            for d in range(4):

                @pl.when(on[d])
                def _():
                    send(which[d], d).wait_send()

        return relay, finish, drain

    spreads = [
        spread(0, erow.at[0], z, 2 * k), spread(1, erow.at[1], z, 2 * k + 1),
        spread(2, epan, jnp.int32(0), jnp.int32(0)),
    ]

    def relay_all(depth):
        for relay, _, _ in spreads:
            relay(depth)

    relay_all(0)
    chain_round(4)
    step(7)
    wait_doubles(3)
    send_doubles(2)
    relay_all(1)
    chain_round(5)
    step(8)

    wait_doubles(2)
    send_doubles(1)
    relay_all(2)
    step(9)
    wait_doubles(1)
    send_doubles(0)
    relay_all(3)
    step(10)
    chain_ends()

    @pl.when(c == 0)
    def _():
        for t in range(4):
            for u in range(2):
                for b in range(2):
                    at = 256 * b + 64 * t + 32 * u
                    rfirst[t, u, :, b * 512 : (b + 1) * 512] = colp[at : at + 32, 512:1024]

    step(11)
    wait_doubles(0)
    go(rcopy(act.at[k], act.at[k], d2_s, d2_r, partner, c))

    relay_all(4)
    for _, finish_spread, _ in spreads:
        finish_spread()

    own_cap.wait()
    for dz, dk in column:
        n = 2 * dz + dk
        rcopy(cap.at[0], capall.at[row_of(4 - dz, 2 - dk)], cp_s.at[n], cp_r.at[n], partner, c).wait_recv()

    def gradients(h, n):
        q = h * 4 + n
        right = jnp.concatenate([act[h, t, :, n].reshape(256, 128) for t in range(4)], axis=0)
        ids = lax.broadcasted_iota(jnp.int32, (64, 1024), 0)
        member = (capall[q] == ids).astype(F32).astype(BF)
        spot = pl.ds(pl.multiple_of(q * 64, 64), 64)
        for src, dst, base in (
            (erow.at[0], grow, 0), (erow.at[1], grow, 1024), (ecol, gcol, 0), (epan, gpan, 0),
        ):
            e8 = src[q]
            left = jnp.concatenate([member * e8[i : i + 1, :] for i in range(8)], axis=0)
            out = dot(left, right).astype(BF)
            for i in range(8):
                dst[spot, base + i * 128 : base + (i + 1) * 128] = out[i * 64 : (i + 1) * 64]

    @pl.loop(0, 2)
    def _(i):
        @pl.when(i == 1)
        def _():
            rcopy(act.at[k], act.at[1 - k], d2_s, d2_r, partner, c).wait_recv()

        for n in range(4):
            gradients((k + i) % 2, n)
            step(12 + 4 * i + n)

    scale = 1.0 / 512.0
    for n in range(2):
        gpt[n * 512 : (n + 1) * 512, :] = gpan[:, n * 512 : (n + 1) * 512].T
    step(20)
    step(21)
    for n in range(4):
        growt[n * 512 : (n + 1) * 512, :] = grow[:, n * 512 : (n + 1) * 512].T

    u1p, q0p = stage.at[pl.ds(0, 512)], stage.at[pl.ds(512, 512)]
    for n in range(2):

        @pl.when(c != 0)
        def _():
            for cols in (slice(n * 512, n * 512 + 256), slice(n * 512 + 256, n * 512 + 512)):
                at = (colp[:, cols].astype(F32) + dot(gpt[...], gcol[:, cols]) * scale).astype(BF)
                atb[:, cols] = at
                u0 = dot(l0[...], at[0:512]).astype(BF)
                u1p[:, cols] = dot(l1[...], at[512:1024])
                q0p[:, cols] = dot(l0t[...], u0)

        step(22 + 2 * n)
        step(23 + 2 * n)

    for u in range(2):
        for t in range(4):

            @pl.when(jnp.logical_and(bits[t] == 0, count > 0))
            def _():
                hop(t, Q01 + u, 0, True).wait_recv()

    for t in range(4):
        for u in range(2):
            for b in range(2):
                at = 256 * b + 64 * t + 32 * u
                r01[at : at + 32, :] = rfirst[t, u, :, b * 512 : (b + 1) * 512]
    a01 = (r01[...].astype(F32) + dot(gpt[0:512, :], gpan[:, 512:1024]) * scale).astype(BF)
    corner = -dot(dot(s0[...], a01).astype(BF), l1t[...])
    w01[...] = corner.astype(BF)
    w01t[...] = corner.T.astype(BF)

    @pl.when(c == 0)
    def _():
        rhsr[0:512, 0:512] = l0t[...]
        rhsr[0:512, 512:1024] = w01[...]
        rhsr[512:1024, 0:512] = jnp.zeros((512, 512), BF)
        rhsr[512:1024, 512:1024] = l1t[...]

    @pl.when(c != 0)
    def _():
        for n in range(4):
            cols = slice(n * 256, n * 256 + 256)
            u1 = (u1p[:, cols] + dot(w01t[...], atb[0:512, cols])).astype(BF)
            rhsr[0:512, cols] = (-(q0p[:, cols] + dot(w01[...], u1))).astype(BF)
            rhsr[512:1024, cols] = (-dot(l1t[...], u1)).astype(BF)

    for n in range(4):
        cols = slice(n * 256, n * 256 + 256)
        own = jnp.where(c == 0, 0.0, gcol[:, cols].astype(F32))
        rhsg[:, cols] = ((own + dot(gpan[...], rhsr[:, cols])) * scale).astype(BF)

    @pl.loop(0, CT)
    def _(q):
        for t in range(4):

            @pl.when(jnp.logical_and(jnp.logical_and(bits[t] == 0, count > 0), jnp.logical_not(is_first(q))))
            def _():
                hop(t, q, 0, False).wait_recv()

        for d in range(4):
            for first in (False, True):

                @pl.when(jnp.logical_and(sends_on[d], is_first(q) == first))
                def _():
                    hop(tree[d], q, d, first).wait_send()

    for copy in sends:
        copy.wait_send()

    @pl.when(h != k)
    def _():
        rcopy(my_act, mine, sa_s.at[0], sa_r.at[half, k], partner, c).wait_send()

    @pl.when(k == 0)
    def _():
        for n in range(4):
            for chain in range(2):

                @pl.when(place_of(chain) < 3)
                def _():
                    along(chain, n).wait_send()

                across(chain, n).wait_send()

    for _, _, drain in spreads:
        drain()


def finish(ridge, growt, rows, rhsg, rhsr, out):
    r = lax.axis_index("row")
    c = lax.axis_index("col")
    n = pl.program_id(0)
    height, width = out.shape
    some = pl.ds(pl.multiple_of(n * height, height), height)
    blank = jnp.logical_and(r * 2048 + n * height < 1024, c > 0)

    @pl.when(blank)
    def _():
        out[...] = jnp.zeros_like(out)

    @pl.when(jnp.logical_not(blank))
    def _():
        for part in range(4):
            cols = slice(part * 256, part * 256 + 256)
            value = dot(growt[some, :], rhsg[:, cols]) + dot(rows[some, :], rhsr[:, cols])
            out[:, cols] = value + jnp.where(c == 0, 0.0, ridge[:, cols])

    @pl.when(jnp.logical_and(r * 2048 + n * height < 512, c == 0))
    def _():
        out[:, 512:1024] = jnp.zeros((height, 512), F32)


def shape(dims, kind):
    return jax.ShapeDtypeStruct(dims, kind)


VM = pl.BlockSpec(memory_space=pltpu.VMEM)
ANY = pl.BlockSpec(memory_space=pl.ANY)
HBM = pl.BlockSpec(memory_space=pltpu.HBM)
DMA = pltpu.SemaphoreType.DMA


def per_device(activations, errors, act_proj, err_proj, lengths, ridge, pivot_inverse):
    vmem = pltpu.VMEM
    half = (512, 512)
    args = [
        pltpu.with_memory_space_constraint(a, pltpu.HBM)
        for a in (activations, errors, act_proj, err_proj, lengths, pivot_inverse, ridge)
    ]
    growt, rows, rhsg, rhsr = pl.pallas_call(
        exchange,
        out_shape=(
            vmem((2048, 512), BF), vmem((2048, 1024), BF), vmem((512, 1024), BF), vmem((1024, 1024), BF)
        ),
        in_specs=[HBM, HBM, HBM, HBM, HBM, HBM, HBM],
        out_specs=(VM,) * 4,
        scratch_shapes=[
            vmem((1024, 512), BF), vmem((1024, 512), BF), vmem((512, 128), BF), vmem((512, 128), BF),
            vmem((1, 64), jnp.int32), vmem((2, 512, 512), F32), vmem((2048, 1024), F32),
            vmem((4, 16, 32, 128), F32), vmem((4, 8, 32, 128), F32), vmem((4, 4, 32, 128), F32),
            vmem((4, 2, 32, 128), F32), vmem((4, 1, 32, 128), F32),
            vmem((4, 16, 128), BF), vmem((8, 1024), BF), vmem((2, 2, 4, 16, 128), BF),
            vmem((2, 4, 16, 4, 16, 128), BF), vmem((2, 8, 8, 1024), BF), vmem((8, 8, 1024), BF),
            vmem((8, 8, 1024), BF), vmem((1, 1, 1024), jnp.int32), vmem((8, 1, 1024), jnp.int32),
            vmem((4, 2, 32, 1024), BF), vmem((1024, 1024), BF),
        ]
        + [vmem(half, BF)] * 5
        + [
            vmem((512, 2048), BF), vmem((512, 1024), BF), vmem((512, 1024), BF),
            vmem((1024, 512), BF),
            vmem((1024, 1024), BF),
        ]
        + [vmem(half, BF)] * 3
        + [
            DMA((4, 4)), DMA((4, 4)), DMA((4, 4)), DMA((4, 4)),
            DMA((4,)), DMA((2, 2)), DMA((8,)), DMA((8,)), DMA((8,)), DMA((8,)),
            DMA((2, 4)), DMA((2, 4)), DMA((2, 4)), DMA((2, 4)),
            DMA((3, 4)), DMA((3, 4)), DMA, DMA,
            DMA((4, CT)), DMA((4, CT)), DMA((8,)), DMA((6,)),
        ],
        compiler_params=pltpu.CompilerParams(
            collective_id=0, has_side_effects=True, vmem_limit_bytes=44 << 20
        ),
        name="exchange",
    )(*args)

    step = 512
    return pl.pallas_call(
        finish,
        out_shape=shape((2048, 1024), F32),
        grid=(2048 // step,),
        in_specs=[
            pl.BlockSpec((step, 1024), lambda n: (n, 0)),
            VM, VM, VM, VM,
        ],
        out_specs=pl.BlockSpec((step, 1024), lambda n: (n, 0)),
        compiler_params=pltpu.CompilerParams(vmem_limit_bytes=20 << 20),
        name="finish",
    )(ridge, *(pltpu.with_memory_space_constraint(a, pltpu.VMEM) for a in (growt, rows, rhsg, rhsr)))


def solution(mesh):
    in_specs = (
        P("row", "col"), P("row", "col"), P("col", None), P("col", None),
        P("row", None), P("row", "col"), P(),
    )
    return jax.shard_map(
        per_device, mesh=mesh, in_specs=in_specs, out_specs=P("row", "col"), check_vma=False
    )
```
